256 devices in a mesh: gx: 8 (over x, core), gy: 32 (over y, z).
Axes of the slice: x: 4, y: 4, z: 8, core: 2. Of those that a mesh axis runs over, the one named last changes fastest.
Arguments:
- features: bfloat16 [65536, 128], P(('gx', 'gy')), may hold values from -6 to 6
- tile_vals: bfloat16 [16384, 128, 128], P(('gx', 'gy')), may hold values from -0.125 to 0.125
- tile_row: int32 [16384], P(('gx', 'gy')), may hold values from 0 to 511, as said below
- tile_col: int32 [16384], P(('gx', 'gy')), may hold values from 0 to 511, as said below
- tile_work: int32 [16384], P(('gx', 'gy')), may hold values from 0 to 16384, as said below
Outputs:
- product: float32 [65536, 128], P(('gx', 'gy'))
- moved_vals: bfloat16 [8192, 128, 128], P(('gx', 'gy'))
- moved_row: int32 [8192], P(('gx', 'gy'))
- moved_col: int32 [8192], P(('gx', 'gy'))
- moved_work: int32 [8192], P(('gx', 'gy'))
The draws below stay inside these ranges and needn't reach their ends.
Inputs may be any that keep to these rules, and one draw needn't show every extreme that they name: `tile_work`: on every device the live slots come first; each gx row of 32 devices holds exactly 1024 live tiles, and in every row one device has all 64 slots live. `tile_row`: A tile held by device (a, b) has a row block owned by a device of gx index a. `tile_col`: A tile held by device (a, b) has a column block owned by a device of gy index b.
All inputs are finite; a program needn't handle non-finite values.
Results may differ from the reference program's by a relative error of at most 0.001.
Values may be sent and summed in bfloat16 or wider, within the bound.
A program may use at most 64 MiB of HBM per device.

```python
import jax
import jax.numpy as jnp
from jax import lax

B = 128
K = 128
VBD = 2
TD = 64
OWN = 32
NB = 512
NV = 65536
NT = 16384
N_GX = 8
N_GY = 32


def skewed_index(key, shape, extent):
    first = jax.random.randint(jax.random.fold_in(key, 11), shape, 0, extent)
    second = jax.random.randint(jax.random.fold_in(key, 12), shape, 0, extent)
    rotate = jax.random.randint(jax.random.fold_in(key, 13), (), 0, extent)
    return (first * second // extent + rotate) % extent


def draw_tile_work(key, part):
    half = N_GY // 2
    delta = jax.random.randint(jax.random.fold_in(key, 1), (N_GX, half), 1 - OWN, OWN)
    forced = jax.random.randint(jax.random.fold_in(key, 2), (N_GX,), 0, half)
    delta = jnp.where(jnp.arange(half)[None, :] == forced[:, None], OWN, delta)
    paired = jnp.concatenate([OWN + delta, OWN - delta], axis=1)
    row_keys = jax.random.split(jax.random.fold_in(key, 3), N_GX)
    counts = jax.vmap(lambda row_key, row: jax.random.permutation(row_key, row))(row_keys, paired)
    slot = jnp.arange(TD, dtype=jnp.int32)[None, None, :]
    amounts = jax.random.randint(jax.random.fold_in(key, 4), (N_GX, N_GY, TD), 1, B * B + 1)
    return jnp.where(slot < counts[:, :, None], amounts, 0).reshape(-1).astype(jnp.int32)


def draw_tile_row(key, part):
    extent = N_GY * VBD
    device = jnp.arange(NT, dtype=jnp.int32) // TD
    outer = device // N_GY
    local = skewed_index(jax.random.fold_in(key, 21), (NT,), extent)
    return (outer * extent + local).astype(jnp.int32)


def draw_tile_col(key, part):
    extent = N_GX * VBD
    device = jnp.arange(NT, dtype=jnp.int32) // TD
    inner = device % N_GY
    local = skewed_index(jax.random.fold_in(key, 31), (NT,), extent)
    return ((local // VBD * N_GY + inner) * VBD + local % VBD).astype(jnp.int32)


def block_scale(key, dims, shards, smallest, high):
    level, own = 1.0, jax.random.fold_in(key, 6)
    for axis_at, blocks in shards:
        draws = jnp.exp(jax.random.uniform(jax.random.fold_in(own, axis_at), (blocks,), jnp.float32, smallest / len(shards), high / len(shards)))
        level = level * jnp.repeat(draws, dims[axis_at] // blocks).reshape([-1 if axis == axis_at else 1 for axis in range(len(dims))])
    return level


def gaussian(key, dims, scale, limit, shards=(), kind=jnp.bfloat16):
    loudness = block_scale(key, dims, shards, -0.22, 0.18) if shards else 1.0
    entries = jax.random.normal(key, dims, jnp.float32) * scale * loudness
    return jnp.minimum(jnp.maximum(entries, -limit), limit).astype(kind)


def setup_inputs(seed: int = 0) -> dict:
    key_of = jax.random.split(jax.random.key(seed), 6)
    features = gaussian(key_of[0], (NV, K), 1.0, 6.0, ((0, 256),))
    tile_vals = gaussian(key_of[1], (NT, B, B), (B * OWN // VBD) ** -0.5, 0.125, ((0, 256),))
    tile_row = draw_tile_row(jax.random.fold_in(key_of[5], 71), 0)
    tile_col = draw_tile_col(jax.random.fold_in(key_of[5], 71), 0)
    tile_work = draw_tile_work(jax.random.fold_in(key_of[5], 71), 0)
    return dict(features=features, tile_vals=tile_vals, tile_row=tile_row, tile_col=tile_col, tile_work=tile_work)


def reference(features, tile_vals, tile_row, tile_col, tile_work):
    devices = N_GX * N_GY
    live = (tile_work > 0).astype(jnp.int32).reshape(N_GX, N_GY, TD)
    counts = jnp.sum(live, axis=2)
    offsets = jnp.cumsum(counts, axis=1) - counts
    position = offsets[:, :, None] + jnp.arange(TD, dtype=jnp.int32)[None, None, :]
    row_index = jnp.arange(N_GX, dtype=jnp.int32)[:, None, None]
    target = (row_index * N_GY + position % N_GY) * OWN + position // N_GY
    target = jnp.where(live > 0, target, devices * OWN).reshape(-1).astype(jnp.int32)
    moved_vals = jnp.zeros((devices * OWN, B, B), jnp.bfloat16).at[target].set(tile_vals, mode="drop")
    moved_row = jnp.zeros((devices * OWN,), jnp.int32).at[target].set(tile_row, mode="drop")
    moved_col = jnp.zeros((devices * OWN,), jnp.int32).at[target].set(tile_col, mode="drop")
    moved_work = jnp.zeros((devices * OWN,), jnp.int32).at[target].set(tile_work, mode="drop")
    pattern = jnp.arange(B * B, dtype=jnp.int32).reshape(B, B)
    blocks = features.reshape(NB, B, K)

    def one_device(total, device):
        begin = (device * TD).astype(jnp.int32)
        values = lax.dynamic_slice_in_dim(tile_vals, begin, TD, 0)
        work = lax.dynamic_slice_in_dim(tile_work, begin, TD, 0)
        rows = lax.dynamic_slice_in_dim(tile_row, begin, TD, 0)
        columns = lax.dynamic_slice_in_dim(tile_col, begin, TD, 0)
        masked = jnp.where(pattern[None, :, :] < work[:, None, None], values, jnp.zeros((), jnp.bfloat16))
        vectors = jnp.take(blocks, columns, axis=0)
        products = jnp.einsum("tij,tjk->tik", masked.astype(jnp.float32), vectors.astype(jnp.float32))
        return total + jax.ops.segment_sum(products, rows, num_segments=NB), None

    summed, unused = lax.scan(one_device, jnp.zeros((NB, B, K), jnp.float32), jnp.arange(devices, dtype=jnp.int32))
    return summed.reshape(NB * B, K), moved_vals, moved_row, moved_col, moved_work
```

```python
import functools

import jax
import jax.numpy as jnp
from jax import lax
from jax.experimental import pallas as pl
from jax.experimental.pallas import tpu as pltpu
from jax.sharding import PartitionSpec as P

NZ = 8
PARTS = (10, 21)
LIMIT = 32000.0
TINY = 1e-30
MESH = pl.DeviceIdType.MESH


def near_first(count):
    return sorted(range(1, count), key=lambda d: (min(d, count - d), d))


def tile_routes(ny, nz):
    pairs = [(dy, dz) for dz in [0, *near_first(nz)] for dy in [0, *near_first(ny)]]
    return pairs[1:]


def whole_wait(ref, sem):
    pltpu.make_async_copy(ref, ref, sem).wait()


def narrowed(value):
    peak = jnp.maximum(jnp.max(jnp.abs(value), axis=0, keepdims=True), TINY)
    coded = jnp.round(value * (LIMIT / peak)).astype(jnp.int32).astype(jnp.int16)
    return coded, peak * (1.0 / LIMIT)


def widened(coded, scale):
    return coded.astype(jnp.int32).astype(jnp.float32) * scale


def kernel(
    sizes,
    feat,
    tiles_hbm,
    row_v,
    col_v,
    work_v,
    col_s,
    work_s,
    chain_s,
    prod,
    moved,
    mrow,
    mcol,
    mwork,
    tiles,
    sendbuf,
    recvbuf,
    xbuf,
    sums,
    metabuf,
    posbuf,
    rowbuf,
    colbuf,
    workbuf,
    yq,
    ys,
    yrecv,
    ysrecv,
    ysum,
    zq,
    zs,
    zrecv,
    zsrecv,
    source,
    sems,
):
    nx, ny, nz = sizes
    peers = ny * nz
    slots = tiles.shape[0]
    vb = feat.shape[0]
    per_row = peers * vb
    per_y = nz * vb
    gx, gy = lax.axis_index("gx"), lax.axis_index("gy")
    y, z = gy // nz, gy % nz
    (tile_in, meta_tx, meta_rx, feat_tx, feat_rx, vals_tx, vals_rx) = (sems.at[i] for i in range(7))
    (y_tx, y_rx, ys_tx, ys_rx, z_tx, z_rx, zs_tx, zs_rx) = (sems.at[7 + i] for i in range(8))

    load = pltpu.make_async_copy(tiles_hbm, tiles, tile_in)
    load.start()

    barrier = pltpu.get_barrier_semaphore()

    def greet_gy(d, carry):
        pl.semaphore_signal(barrier, inc=1, device_id={"gy": (gy + d) % peers}, device_id_type=MESH)
        return carry

    def greet_gx(d, carry):
        pl.semaphore_signal(barrier, inc=1, device_id={"gx": (gx + d) % nx}, device_id_type=MESH)
        return carry

    lax.fori_loop(1, peers, greet_gy, 0)
    lax.fori_loop(1, nx, greet_gx, 0)

    metabuf[gy] = jnp.zeros(metabuf.shape[1:], jnp.int32)
    metabuf[gy, 0:1, 0:slots] = row_v[...]
    metabuf[gy, 1:2, 0:slots] = col_v[...]
    metabuf[gy, 2:3, 0:slots] = work_v[...]
    live = jnp.sum((work_v[...] > 0).astype(jnp.int32), axis=1, keepdims=True)
    metabuf[gy, 3:4, :] = jnp.broadcast_to(live, (1, metabuf.shape[2]))
    xbuf[pl.ds(gx * vb, vb)] = feat[...]

    pl.semaphore_wait(barrier, peers - 1 + nx - 1)

    def send_meta(d, carry):
        pltpu.make_async_remote_copy(
            src_ref=metabuf.at[gy],
            dst_ref=metabuf.at[gy],
            send_sem=meta_tx,
            recv_sem=meta_rx,
            device_id={"gy": (gy + d) % peers},
            device_id_type=MESH,
        ).start()
        return carry

    lax.fori_loop(1, peers, send_meta, 0)

    def send_feat(d, carry):
        pltpu.make_async_remote_copy(
            src_ref=feat,
            dst_ref=xbuf.at[pl.ds(gx * vb, vb)],
            send_sem=feat_tx,
            recv_sem=feat_rx,
            device_id={"gx": (gx + d) % nx},
            device_id_type=MESH,
        ).start()
        return carry

    lax.fori_loop(1, nx, send_feat, 0)

    load.wait()
    whole_wait(metabuf.at[pl.ds(0, peers - 1)], meta_rx)

    def before(c, total):
        return total + jnp.where(c < gy, metabuf[c], 0)

    counted = lax.fori_loop(0, peers, before, jnp.zeros(metabuf.shape[1:], jnp.int32))
    first = jnp.max(counted[3:4, :])

    def arrange(t, carry):
        j = (t - first) & (peers - 1)
        sendbuf[2 * t] = tiles[j]
        sendbuf[2 * t + 1] = tiles[j + peers]
        return carry

    lax.fori_loop(0, peers, arrange, 0)

    routes = tile_routes(ny, nz)

    def send_tiles(begin, end):
        for dy, dz in routes[begin:end]:
            to = (y + dy) % ny * nz + (z + dz) % nz
            pltpu.make_async_remote_copy(
                src_ref=sendbuf.at[pl.ds(2 * to, 2)],
                dst_ref=recvbuf.at[pl.ds(2 * gy, 2)],
                send_sem=vals_tx,
                recv_sem=vals_rx,
                device_id={"gy": to},
                device_id_type=MESH,
            ).start()

    recvbuf[pl.ds(2 * gy, 2)] = sendbuf[pl.ds(2 * gy, 2)]
    cuts = [len(routes) * c // 31 for c in PARTS]
    send_tiles(0, cuts[0])

    whole_wait(xbuf.at[pl.ds(0, (nx - 1) * vb)], feat_rx)
    order = tiles.shape[1]
    pattern = lax.broadcasted_iota(jnp.int32, (order, order), 0) * order + lax.broadcasted_iota(
        jnp.int32, (order, order), 1
    )

    def multiply(t, carry):
        col = col_s[t]
        at = col // per_row * vb + col % vb
        kept = jnp.where(pattern < work_s[t], tiles[t].astype(jnp.float32), 0.0)
        sums[t] = jnp.dot(
            kept.astype(jnp.bfloat16), xbuf[at], preferred_element_type=jnp.float32
        )
        return carry

    lax.fori_loop(0, slots, multiply, 0, unroll=4)

    def chain(t, carry):
        prev = chain_s[t]
        sums[t] = sums[t] + jnp.where(prev >= 0, sums[jnp.maximum(prev, 0)], 0.0)
        return carry

    lax.fori_loop(0, slots, chain, 0)

    def partial(r):
        last = chain_s[slots + r]
        return jnp.where(last >= 0, sums[jnp.maximum(last, 0)], 0.0)

    def send_y(dy):
        to = (y + dy) % ny * nz + z
        for src, dst, tx, rx in ((yq, yrecv, y_tx, y_rx), (ys, ysrecv, ys_tx, ys_rx)):
            pltpu.make_async_remote_copy(
                src_ref=src.at[dy - 1],
                dst_ref=dst.at[dy - 1],
                send_sem=tx,
                recv_sem=rx,
                device_id={"gy": to},
                device_id_type=MESH,
            ).start()

    for dy in range(1, ny):
        base = (y + dy) % ny * per_y

        def code_y(k, carry, dy=dy, base=base):
            coded, scale = narrowed(partial(base + k))
            yq[dy - 1, k] = coded
            ys[dy - 1, pl.ds(k, 1), :] = scale
            return carry

        lax.fori_loop(0, per_y, code_y, 0, unroll=2)
        if dy > 1:
            send_y(dy - 1)

    def own_y(k, carry):
        ysum[k] = partial(y * per_y + k)
        return carry

    lax.fori_loop(0, per_y, own_y, 0)
    send_y(ny - 1)
    send_tiles(cuts[0], cuts[1])

    whole_wait(yrecv, y_rx)
    whole_wait(ysrecv, ys_rx)

    def add_y(k, carry):
        total = ysum[k]
        for dy in range(1, ny):
            total = total + widened(yrecv[dy - 1, k], ysrecv[dy - 1, pl.ds(k, 1), :])
        ysum[k] = total
        return carry

    lax.fori_loop(0, per_y, add_y, 0)

    def send_z(dz):
        to = y * nz + (z + dz) % nz
        for src, dst, tx, rx in ((zq, zrecv, z_tx, z_rx), (zs, zsrecv, zs_tx, zs_rx)):
            pltpu.make_async_remote_copy(
                src_ref=src.at[dz - 1],
                dst_ref=dst.at[dz - 1],
                send_sem=tx,
                recv_sem=rx,
                device_id={"gy": to},
                device_id_type=MESH,
            ).start()

    def code_z(i, carry):
        dz, v = i // vb + 1, i % vb
        coded, scale = narrowed(ysum[(z + dz) % nz * vb + v])
        zq[dz - 1, v] = coded
        zs[dz - 1, pl.ds(v, 1), :] = scale
        return carry

    lax.fori_loop(0, (nz - 1) * vb, code_z, 0, unroll=2)
    for v in range(vb):
        prod[v] = ysum[z * vb + v]
    for dz in near_first(nz)[::-1]:
        send_z(dz)
    send_tiles(cuts[1], len(routes))

    lane = lax.broadcasted_iota(jnp.int32, (1, posbuf.shape[1]), 1)
    offset = jnp.zeros((1, posbuf.shape[1]), jnp.int32)
    for c in range(peers):
        one = metabuf[c]
        rowbuf[c : c + 1, :] = one[0:1, :]
        colbuf[c : c + 1, :] = one[1:2, :]
        workbuf[c : c + 1, :] = one[2:3, :]
        posbuf[c : c + 1, :] = jnp.where(one[2:3, :] > 0, offset + lane, -1)
        offset = offset + one[3:4, :]

    lanes = posbuf.shape
    origin = 2 * lax.broadcasted_iota(jnp.int32, lanes, 0) + (
        lax.broadcasted_iota(jnp.int32, lanes, 1) >= peers
    ).astype(jnp.int32)

    def place(q, carry):
        hit = posbuf[...] == q * peers + gy

        def picked(values):
            return jnp.sum(jnp.where(hit, values, 0))

        mrow[q] = picked(rowbuf[...])
        mcol[q] = picked(colbuf[...])
        mwork[q] = picked(workbuf[...])
        source[q] = picked(origin)
        return carry

    lax.fori_loop(0, slots // 2, place, 0)

    whole_wait(zrecv, z_rx)
    whole_wait(zsrecv, zs_rx)
    for v in range(vb):

        def add_z(d, total, v=v):
            return total + widened(zrecv[d, v], zsrecv[d, v : v + 1, :])

        prod[v] = lax.fori_loop(0, nz - 1, add_z, prod[v])

    whole_wait(recvbuf.at[pl.ds(0, 2 * (peers - 1))], vals_rx)

    def settle(q, carry):
        moved[q] = jnp.where(mwork[q] > 0, recvbuf[source[q]].astype(jnp.float32), 0.0).astype(
            moved.dtype
        )
        return carry

    lax.fori_loop(0, slots // 2, settle, 0, unroll=2)

    whole_wait(metabuf.at[pl.ds(0, peers - 1)], meta_tx)
    whole_wait(xbuf.at[pl.ds(0, (nx - 1) * vb)], feat_tx)
    whole_wait(recvbuf.at[pl.ds(0, 2 * (peers - 1))], vals_tx)
    whole_wait(yrecv, y_tx)
    whole_wait(ysrecv, ys_tx)
    whole_wait(zrecv, z_tx)
    whole_wait(zsrecv, zs_tx)


def on_device(sizes, features, tile_vals, tile_row, tile_col, tile_work):
    nx, ny, nz = sizes
    peers = ny * nz
    slots, order, _ = tile_vals.shape
    width = features.shape[1]
    vb = features.shape[0] // order
    local = tile_row - lax.axis_index("gx") * peers * vb
    index = jnp.arange(slots, dtype=jnp.int32)
    wanted = jnp.concatenate([local, jnp.arange(peers * vb, dtype=jnp.int32)])
    until = jnp.concatenate([index, jnp.full((peers * vb,), slots, jnp.int32)])
    found = (wanted[:, None] == local[None, :]) & (index[None, :] < until[:, None])
    chain = jnp.max(jnp.where(found, index[None, :], -1), axis=1)
    per_y = nz * vb
    bf16, f32, i32, i16 = jnp.bfloat16, jnp.float32, jnp.int32, jnp.int16
    vmem, smem = pltpu.VMEM, pltpu.SMEM
    in_vmem, in_smem = pl.BlockSpec(memory_space=vmem), pl.BlockSpec(memory_space=smem)
    prod, moved, mrow, mcol, mwork = pl.pallas_call(
        functools.partial(kernel, sizes),
        out_shape=(
            jax.ShapeDtypeStruct((vb, order, width), f32),
            jax.ShapeDtypeStruct((slots // 2, order, order), bf16),
            *[jax.ShapeDtypeStruct((slots // 2,), i32)] * 3,
        ),
        in_specs=[
            in_vmem,
            pl.BlockSpec(memory_space=pl.ANY),
            in_vmem,
            in_vmem,
            in_vmem,
            in_smem,
            in_smem,
            in_smem,
        ],
        out_specs=(in_vmem, in_vmem, in_smem, in_smem, in_smem),
        scratch_shapes=[
            vmem((slots, order, order), bf16),
            vmem((slots, order, order), bf16),
            vmem((slots, order, order), bf16),
            vmem((nx * vb, order, width), bf16),
            vmem((slots, order, width), f32),
            vmem((peers, 8, 128), i32),
            *[vmem((peers, 128), i32)] * 4,
            vmem((ny - 1, per_y, order, width), i16),
            vmem((ny - 1, per_y, width), f32),
            vmem((ny - 1, per_y, order, width), i16),
            vmem((ny - 1, per_y, width), f32),
            vmem((per_y, order, width), f32),
            vmem((nz - 1, vb, order, width), i16),
            vmem((nz - 1, 8, width), f32),
            vmem((nz - 1, vb, order, width), i16),
            vmem((nz - 1, 8, width), f32),
            smem((slots // 2,), i32),
            pltpu.SemaphoreType.DMA((15,)),
        ],
        compiler_params=pltpu.CompilerParams(
            collective_id=0, has_side_effects=True, vmem_limit_bytes=40 * 2**20
        ),
    )(
        features.reshape(vb, order, width),
        tile_vals,
        tile_row.reshape(1, slots),
        tile_col.reshape(1, slots),
        tile_work.reshape(1, slots),
        tile_col,
        tile_work,
        chain,
    )
    return prod.reshape(vb * order, width), moved, mrow, mcol, mwork


def solution(mesh):
    nx, peers = mesh.shape["gx"], mesh.shape["gy"]
    nz = min(NZ, peers // 2)
    both = ("gx", "gy")
    specs = (P(both, None), P(both, None, None), P(both), P(both), P(both))
    return jax.shard_map(
        functools.partial(on_device, (nx, peers // nz, nz)),
        mesh=mesh,
        in_specs=specs,
        out_specs=specs,
        check_vma=False,
    )
```

```python
import functools

import jax
import jax.numpy as jnp
from jax import lax
from jax.experimental import pallas as pl
from jax.experimental.pallas import tpu as pltpu
from jax.sharding import PartitionSpec as P

NZ = 8
FIRST = 16
LIMIT = 32000.0
TINY = 1e-30
MESH = pl.DeviceIdType.MESH


def near_first(count):
    return sorted(range(1, count), key=lambda d: (min(d, count - d), d))


def tile_routes(ny, nz):
    pairs = [(dy, dz) for dz in [0, *near_first(nz)] for dy in [0, *near_first(ny)]]
    return pairs[:0:-1]


def whole_wait(ref, sem):
    pltpu.make_async_copy(ref, ref, sem).wait()


def narrowed(value):
    peak = jnp.maximum(jnp.max(jnp.abs(value), axis=0, keepdims=True), TINY)
    coded = jnp.round(value * (LIMIT / peak)).astype(jnp.int32).astype(jnp.int16)
    return coded, peak * (1.0 / LIMIT)


def widened(coded, scale):
    return coded.astype(jnp.int32).astype(jnp.float32) * scale


def kernel(
    sizes,
    feat_hbm,
    tiles_hbm,
    row_hbm,
    col_hbm,
    work_hbm,
    row_line,
    col_line,
    work_line,
    prod,
    moved,
    mrow,
    mcol,
    mwork,
    row_s,
    col_s,
    work_s,
    chain_s,
    row_v,
    col_v,
    work_v,
    chain_v,
    tiles,
    sendbuf,
    recvbuf,
    xbuf,
    sums,
    metabuf,
    posbuf,
    rowbuf,
    colbuf,
    workbuf,
    yq,
    ys,
    yrecv,
    ysrecv,
    ysum,
    zq,
    zs,
    zrecv,
    zsrecv,
    source,
    sems,
):
    nx, ny, nz = sizes
    peers = ny * nz
    slots = tiles.shape[0]
    vb = feat_hbm.shape[0]
    per_row = peers * vb
    per_y = nz * vb
    gx, gy = lax.axis_index("gx"), lax.axis_index("gy")
    y, z = gy // nz, gy % nz
    (tile_in, meta_tx, meta_rx, feat_tx, feat_rx, vals_tx, vals_rx) = (sems.at[i] for i in range(7))
    (y_tx, y_rx, ys_tx, ys_rx, z_tx, z_rx, zs_tx, zs_rx) = (sems.at[7 + i] for i in range(8))

    own_x = xbuf.at[pl.ds(gx * vb, vb)]
    small = [
        pltpu.make_async_copy(src, dst, sems.at[15 + i])
        for i, (src, dst) in enumerate(
            (
                (row_hbm, row_s),
                (row_line, row_v),
                (work_line, work_v),
                (col_line, col_v),
                (feat_hbm, own_x),
                (col_hbm, col_s),
                (work_hbm, work_s),
            )
        )
    ]
    for copy in small:
        copy.start()
    load = pltpu.make_async_copy(tiles_hbm, tiles, tile_in)
    load.start()

    barrier = pltpu.get_barrier_semaphore()

    def greet_gy(d, carry):
        pl.semaphore_signal(barrier, inc=1, device_id={"gy": (gy + d) % peers}, device_id_type=MESH)
        return carry

    def greet_gx(d, carry):
        pl.semaphore_signal(barrier, inc=1, device_id={"gx": (gx + d) % nx}, device_id_type=MESH)
        return carry

    lax.fori_loop(1, peers, greet_gy, 0)
    lax.fori_loop(1, nx, greet_gx, 0)

    for copy in small:
        copy.wait()
    metabuf[gy] = jnp.zeros(metabuf.shape[1:], jnp.int32)
    metabuf[gy, 0:1, 0:slots] = row_v[...]
    metabuf[gy, 1:2, 0:slots] = col_v[...]
    metabuf[gy, 2:3, 0:slots] = work_v[...]
    live = jnp.sum((work_v[...] > 0).astype(jnp.int32), axis=1, keepdims=True)
    metabuf[gy, 3:4, :] = jnp.broadcast_to(live, (1, metabuf.shape[2]))

    lane = lax.broadcasted_iota(jnp.int32, (1, chain_v.shape[1]), 1)
    chain_v[...] = lane - slots
    chain_v[0:1, 0:slots] = row_v[...] - gx * per_row
    wanted = chain_v[...]
    until = jnp.where(lane < slots, lane, slots)

    def link(t, latest):
        return jnp.where((wanted == row_s[t] - gx * per_row) & (t < until), t, latest)

    chain_v[...] = lax.fori_loop(0, slots, link, jnp.full(lane.shape, -1, jnp.int32), unroll=4)
    table = pltpu.make_async_copy(chain_v, chain_s, sems.at[22])
    table.start()

    pl.semaphore_wait(barrier, peers - 1 + nx - 1)

    def send_meta(d, carry):
        pltpu.make_async_remote_copy(
            src_ref=metabuf.at[gy],
            dst_ref=metabuf.at[gy],
            send_sem=meta_tx,
            recv_sem=meta_rx,
            device_id={"gy": (gy + d) % peers},
            device_id_type=MESH,
        ).start()
        return carry

    lax.fori_loop(1, peers, send_meta, 0)

    def send_feat(d, carry):
        pltpu.make_async_remote_copy(
            src_ref=own_x,
            dst_ref=own_x,
            send_sem=feat_tx,
            recv_sem=feat_rx,
            device_id={"gx": (gx + d) % nx},
            device_id_type=MESH,
        ).start()
        return carry

    lax.fori_loop(1, nx, send_feat, 0)

    load.wait()
    whole_wait(metabuf.at[pl.ds(0, peers - 1)], meta_rx)

    def before(c, total):
        return total + jnp.where(c < gy, metabuf[c], 0)

    counted = lax.fori_loop(0, peers, before, jnp.zeros(metabuf.shape[1:], jnp.int32))
    first = jnp.max(counted[3:4, :])

    def arrange(t, carry):
        j = (t - first) & (peers - 1)
        sendbuf[2 * t] = tiles[j]
        sendbuf[2 * t + 1] = tiles[j + peers]
        return carry

    lax.fori_loop(0, peers, arrange, 0)

    routes = tile_routes(ny, nz)

    def send_tiles(begin, end):
        for dy, dz in routes[begin:end]:
            to = (y + dy) % ny * nz + (z + dz) % nz
            pltpu.make_async_remote_copy(
                src_ref=sendbuf.at[pl.ds(2 * to, 2)],
                dst_ref=recvbuf.at[pl.ds(2 * gy, 2)],
                send_sem=vals_tx,
                recv_sem=vals_rx,
                device_id={"gy": to},
                device_id_type=MESH,
            ).start()

    recvbuf[pl.ds(2 * gy, 2)] = sendbuf[pl.ds(2 * gy, 2)]
    cut = len(routes) * FIRST // 31
    send_tiles(0, cut)
    table.wait()

    whole_wait(xbuf.at[pl.ds(0, (nx - 1) * vb)], feat_rx)
    order = tiles.shape[1]
    pattern = lax.broadcasted_iota(jnp.int32, (order, order), 0) * order + lax.broadcasted_iota(
        jnp.int32, (order, order), 1
    )

    def multiply(t, carry):
        col = col_s[t]
        at = col // per_row * vb + col % vb
        kept = jnp.where(pattern < work_s[t], tiles[t].astype(jnp.float32), 0.0)
        sums[t] = jnp.dot(
            kept.astype(jnp.bfloat16), xbuf[at], preferred_element_type=jnp.float32
        )
        return carry

    lax.fori_loop(0, slots, multiply, 0, unroll=4)

    def chain(t, carry):
        prev = chain_s[0, t]
        sums[t] = sums[t] + jnp.where(prev >= 0, sums[jnp.maximum(prev, 0)], 0.0)
        return carry

    lax.fori_loop(0, slots, chain, 0)

    def partial(r):
        last = chain_s[0, slots + r]
        return jnp.where(last >= 0, sums[jnp.maximum(last, 0)], 0.0)

    def send_y(dy):
        to = (y + dy) % ny * nz + z
        for src, dst, tx, rx in ((yq, yrecv, y_tx, y_rx), (ys, ysrecv, ys_tx, ys_rx)):
            pltpu.make_async_remote_copy(
                src_ref=src.at[dy - 1],
                dst_ref=dst.at[dy - 1],
                send_sem=tx,
                recv_sem=rx,
                device_id={"gy": to},
                device_id_type=MESH,
            ).start()

    for dy in range(1, ny):
        base = (y + dy) % ny * per_y

        def code_y(k, carry, dy=dy, base=base):
            coded, scale = narrowed(partial(base + k))
            yq[dy - 1, k] = coded
            ys[dy - 1, pl.ds(k, 1), :] = scale
            return carry

        lax.fori_loop(0, per_y, code_y, 0, unroll=2)
        if dy > 1:
            send_y(dy - 1)

    def own_y(k, carry):
        ysum[k] = partial(y * per_y + k)
        return carry

    lax.fori_loop(0, per_y, own_y, 0)
    send_y(ny - 1)
    send_tiles(cut, len(routes))

    whole_wait(yrecv, y_rx)
    whole_wait(ysrecv, ys_rx)

    def add_y(k, carry):
        total = ysum[k]
        for dy in range(1, ny):
            total = total + widened(yrecv[dy - 1, k], ysrecv[dy - 1, pl.ds(k, 1), :])
        ysum[k] = total
        return carry

    lax.fori_loop(0, per_y, add_y, 0)

    def send_z(dz):
        to = y * nz + (z + dz) % nz
        for src, dst, tx, rx in ((zq, zrecv, z_tx, z_rx), (zs, zsrecv, zs_tx, zs_rx)):
            pltpu.make_async_remote_copy(
                src_ref=src.at[dz - 1],
                dst_ref=dst.at[dz - 1],
                send_sem=tx,
                recv_sem=rx,
                device_id={"gy": to},
                device_id_type=MESH,
            ).start()

    def code_z(i, carry):
        dz, v = i // vb + 1, i % vb
        coded, scale = narrowed(ysum[(z + dz) % nz * vb + v])
        zq[dz - 1, v] = coded
        zs[dz - 1, pl.ds(v, 1), :] = scale
        return carry

    lax.fori_loop(0, (nz - 1) * vb, code_z, 0, unroll=2)
    for v in range(vb):
        prod[v] = ysum[z * vb + v]
    for dz in near_first(nz)[::-1]:
        send_z(dz)

    offset = jnp.zeros((1, posbuf.shape[1]), jnp.int32)
    for c in range(peers):
        one = metabuf[c]
        rowbuf[c : c + 1, :] = one[0:1, :]
        colbuf[c : c + 1, :] = one[1:2, :]
        workbuf[c : c + 1, :] = one[2:3, :]
        posbuf[c : c + 1, :] = jnp.where(one[2:3, :] > 0, offset + lane, -1)
        offset = offset + one[3:4, :]

    lanes = posbuf.shape
    origin = 2 * lax.broadcasted_iota(jnp.int32, lanes, 0) + (
        lax.broadcasted_iota(jnp.int32, lanes, 1) >= peers
    ).astype(jnp.int32)

    def place(q, carry):
        hit = posbuf[...] == q * peers + gy

        def picked(values):
            return jnp.sum(jnp.where(hit, values, 0))

        mrow[q] = picked(rowbuf[...])
        mcol[q] = picked(colbuf[...])
        mwork[q] = picked(workbuf[...])
        source[q] = picked(origin)
        return carry

    lax.fori_loop(0, slots // 2, place, 0)

    whole_wait(zrecv, z_rx)
    whole_wait(zsrecv, zs_rx)
    for v in range(vb):

        def add_z(d, total, v=v):
            return total + widened(zrecv[d, v], zsrecv[d, v : v + 1, :])

        prod[v] = lax.fori_loop(0, nz - 1, add_z, prod[v])

    whole_wait(recvbuf.at[pl.ds(0, 2 * (peers - 1))], vals_rx)

    def settle(q, carry):
        moved[q] = jnp.where(mwork[q] > 0, recvbuf[source[q]].astype(jnp.float32), 0.0).astype(
            moved.dtype
        )
        return carry

    lax.fori_loop(0, slots // 2, settle, 0, unroll=2)

    whole_wait(metabuf.at[pl.ds(0, peers - 1)], meta_tx)
    whole_wait(xbuf.at[pl.ds(0, (nx - 1) * vb)], feat_tx)
    whole_wait(recvbuf.at[pl.ds(0, 2 * (peers - 1))], vals_tx)
    whole_wait(yrecv, y_tx)
    whole_wait(ysrecv, ys_tx)
    whole_wait(zrecv, z_tx)
    whole_wait(zsrecv, zs_tx)


def on_device(sizes, features, tile_vals, tile_row, tile_col, tile_work):
    nx, ny, nz = sizes
    peers = ny * nz
    slots, order, _ = tile_vals.shape
    width = features.shape[1]
    vb = features.shape[0] // order
    per_y = nz * vb
    bf16, f32, i32, i16 = jnp.bfloat16, jnp.float32, jnp.int32, jnp.int16
    vmem, smem = pltpu.VMEM, pltpu.SMEM
    in_vmem, in_smem = pl.BlockSpec(memory_space=vmem), pl.BlockSpec(memory_space=smem)
    prod, moved, mrow, mcol, mwork = pl.pallas_call(
        functools.partial(kernel, sizes),
        out_shape=(
            jax.ShapeDtypeStruct((vb, order, width), f32),
            jax.ShapeDtypeStruct((slots // 2, order, order), bf16),
            *[jax.ShapeDtypeStruct((slots // 2,), i32)] * 3,
        ),
        in_specs=[pl.BlockSpec(memory_space=pltpu.HBM)] * 8,
        out_specs=(in_vmem, in_vmem, in_smem, in_smem, in_smem),
        scratch_shapes=[
            *[smem((slots,), i32)] * 3,
            smem((1, slots + peers * vb), i32),
            *[vmem((1, slots), i32)] * 3,
            vmem((1, slots + peers * vb), i32),
            vmem((slots, order, order), bf16),
            vmem((slots, order, order), bf16),
            vmem((slots, order, order), bf16),
            vmem((nx * vb, order, width), bf16),
            vmem((slots, order, width), f32),
            vmem((peers, 8, 128), i32),
            *[vmem((peers, 128), i32)] * 4,
            vmem((ny - 1, per_y, order, width), i16),
            vmem((ny - 1, per_y, width), f32),
            vmem((ny - 1, per_y, order, width), i16),
            vmem((ny - 1, per_y, width), f32),
            vmem((per_y, order, width), f32),
            vmem((nz - 1, vb, order, width), i16),
            vmem((nz - 1, 8, width), f32),
            vmem((nz - 1, vb, order, width), i16),
            vmem((nz - 1, 8, width), f32),
            smem((slots // 2,), i32),
            pltpu.SemaphoreType.DMA((23,)),
        ],
        compiler_params=pltpu.CompilerParams(
            collective_id=0, has_side_effects=True, vmem_limit_bytes=67043328
        ),
    )(
        features.reshape(vb, order, width),
        tile_vals,
        tile_row,
        tile_col,
        tile_work,
        tile_row.reshape(1, slots),
        tile_col.reshape(1, slots),
        tile_work.reshape(1, slots),
    )
    return prod.reshape(vb * order, width), moved, mrow, mcol, mwork


def solution(mesh):
    nx, peers = mesh.shape["gx"], mesh.shape["gy"]
    nz = min(NZ, peers // 2)
    both = ("gx", "gy")
    specs = (P(both, None), P(both, None, None), P(both), P(both), P(both))
    return jax.shard_map(
        functools.partial(on_device, (nx, peers // nz, nz)),
        mesh=mesh,
        in_specs=specs,
        out_specs=specs,
        check_vma=False,
    )
```

```python
import functools

import jax
import jax.numpy as jnp
from jax import lax
from jax.experimental import pallas as pl
from jax.experimental.pallas import tpu as pltpu
from jax.sharding import PartitionSpec as P

NZ = 8
LIMIT = 32000.0
TINY = 1e-30
MESH = pl.DeviceIdType.MESH


def near_first(count):
    return sorted(range(1, count), key=lambda d: (min(d, count - d), d))


def tile_routes(ny, nz):
    pairs = [(dy, dz) for dy in [0, *near_first(ny)] for dz in [0, *near_first(nz)]]
    return pairs[:0:-1]


def z_groups(nz):
    if nz < 8:
        return [*near_first(nz)[::-1], 0]
    return [4, 3, nz - 3, 1, nz - 1, 2, nz - 2, 0]


def z_route(dz, nz):
    hop = {3: 1, 4: 2, nz - 3: nz - 1}.get(dz, dz) if nz == 8 else dz
    return hop, dz - 1


def collected(dz, nz):
    return {2: (4, 3), nz - 2: (nz - 3,)}.get(dz, ()) if nz == 8 else ()


def whole_wait(ref, sem):
    pltpu.make_async_copy(ref, ref, sem).wait()


def narrowed(value):
    peak = jnp.maximum(jnp.max(jnp.abs(value), axis=0, keepdims=True), TINY)
    coded = jnp.round(value * (LIMIT / peak)).astype(jnp.int32).astype(jnp.int16)
    return coded, peak * (1.0 / LIMIT)


def widened(coded, scale):
    return coded.astype(jnp.int32).astype(jnp.float32) * scale


def kernel(
    sizes,
    feat_hbm,
    tiles_hbm,
    row_hbm,
    col_hbm,
    work_hbm,
    row_line,
    col_line,
    work_line,
    prod,
    moved,
    mrow,
    mcol,
    mwork,
    row_s,
    col_s,
    work_s,
    chain_s,
    row_v,
    col_v,
    work_v,
    chain_v,
    tiles,
    sendbuf,
    recvbuf,
    xbuf,
    sums,
    metabuf,
    posbuf,
    rowbuf,
    colbuf,
    workbuf,
    yq,
    ys,
    yrecv,
    ysrecv,
    zq,
    zs,
    zrecv,
    zsrecv,
    source,
    sems,
    y_tx,
    y_rx,
    z_tx,
    z_rx,
):
    nx, ny, nz = sizes
    peers = ny * nz
    slots = tiles.shape[0]
    vb = feat_hbm.shape[0]
    per_row = peers * vb
    per_y = nz * vb
    gx, gy = lax.axis_index("gx"), lax.axis_index("gy")
    y, z = gy // nz, gy % nz
    (tile_in, meta_tx, meta_rx, feat_tx, feat_rx, vals_tx, vals_rx) = (sems.at[i] for i in range(7))

    own_x = xbuf.at[pl.ds(gx * vb, vb)]
    small = [
        pltpu.make_async_copy(src, dst, sems.at[7 + i])
        for i, (src, dst) in enumerate(
            (
                (row_hbm, row_s),
                (row_line, row_v),
                (work_line, work_v),
                (col_line, col_v),
                (feat_hbm, own_x),
                (col_hbm, col_s),
                (work_hbm, work_s),
            )
        )
    ]
    for copy in small:
        copy.start()
    load = pltpu.make_async_copy(tiles_hbm, tiles, tile_in)
    load.start()

    barrier = pltpu.get_barrier_semaphore()

    def greet_gy(d, carry):
        pl.semaphore_signal(barrier, inc=1, device_id={"gy": (gy + d) % peers}, device_id_type=MESH)
        return carry

    def greet_gx(d, carry):
        pl.semaphore_signal(barrier, inc=1, device_id={"gx": (gx + d) % nx}, device_id_type=MESH)
        return carry

    lax.fori_loop(1, peers, greet_gy, 0)
    lax.fori_loop(1, nx, greet_gx, 0)

    for copy in small:
        copy.wait()
    metabuf[gy] = jnp.zeros(metabuf.shape[1:], jnp.int32)
    metabuf[gy, 0:1, 0:slots] = row_v[...]
    metabuf[gy, 1:2, 0:slots] = col_v[...]
    metabuf[gy, 2:3, 0:slots] = work_v[...]
    live = jnp.sum((work_v[...] > 0).astype(jnp.int32), axis=1, keepdims=True)
    metabuf[gy, 3:4, :] = jnp.broadcast_to(live, (1, metabuf.shape[2]))

    lane = lax.broadcasted_iota(jnp.int32, (1, chain_v.shape[1]), 1)
    chain_v[...] = lane - slots
    chain_v[0:1, 0:slots] = row_v[...] - gx * per_row
    wanted = chain_v[...]
    until = jnp.where(lane < slots, lane, slots)

    def link(t, latest):
        return jnp.where((wanted == row_s[t] - gx * per_row) & (t < until), t, latest)

    chain_v[...] = lax.fori_loop(0, slots, link, jnp.full(lane.shape, -1, jnp.int32), unroll=4)
    table = pltpu.make_async_copy(chain_v, chain_s, sems.at[14])
    table.start()

    pl.semaphore_wait(barrier, peers - 1 + nx - 1)

    def send_meta(d, carry):
        pltpu.make_async_remote_copy(
            src_ref=metabuf.at[gy],
            dst_ref=metabuf.at[gy],
            send_sem=meta_tx,
            recv_sem=meta_rx,
            device_id={"gy": (gy + d) % peers},
            device_id_type=MESH,
        ).start()
        return carry

    lax.fori_loop(1, peers, send_meta, 0)

    def send_feat(d, carry):
        pltpu.make_async_remote_copy(
            src_ref=own_x,
            dst_ref=own_x,
            send_sem=feat_tx,
            recv_sem=feat_rx,
            device_id={"gx": (gx + d) % nx},
            device_id_type=MESH,
        ).start()
        return carry

    lax.fori_loop(1, nx, send_feat, 0)

    load.wait()
    whole_wait(metabuf.at[pl.ds(0, peers - 1)], meta_rx)

    def before(c, total):
        return total + jnp.where(c < gy, metabuf[c], 0)

    counted = lax.fori_loop(0, peers, before, jnp.zeros(metabuf.shape[1:], jnp.int32))
    first = jnp.max(counted[3:4, :])

    def arrange(t, carry):
        j = (t - first) & (peers - 1)
        sendbuf[2 * t] = tiles[j]
        sendbuf[2 * t + 1] = tiles[j + peers]
        return carry

    lax.fori_loop(0, peers, arrange, 0)

    routes = tile_routes(ny, nz)

    def send_tiles(dy, dz):
        to = (y + dy) % ny * nz + (z + dz) % nz
        pltpu.make_async_remote_copy(
            src_ref=sendbuf.at[pl.ds(2 * to, 2)],
            dst_ref=recvbuf.at[pl.ds(2 * gy, 2)],
            send_sem=vals_tx,
            recv_sem=vals_rx,
            device_id={"gy": to},
            device_id_type=MESH,
        ).start()

    recvbuf[pl.ds(2 * gy, 2)] = sendbuf[pl.ds(2 * gy, 2)]
    for dy, dz in routes:
        send_tiles(dy, dz)
    table.wait()
    whole_wait(xbuf.at[pl.ds(0, (nx - 1) * vb)], feat_rx)
    order = tiles.shape[1]
    pattern = lax.broadcasted_iota(jnp.int32, (order, order), 0) * order + lax.broadcasted_iota(
        jnp.int32, (order, order), 1
    )

    def multiply(t, carry):
        col = col_s[t]
        at = col // per_row * vb + col % vb
        kept = jnp.where(pattern < work_s[t], tiles[t].astype(jnp.float32), 0.0)
        sums[t] = jnp.dot(
            kept.astype(jnp.bfloat16), xbuf[at], preferred_element_type=jnp.float32
        )
        return carry

    lax.fori_loop(0, slots, multiply, 0, unroll=4)

    def chain(t, carry):
        prev = chain_s[0, t]
        sums[t] = sums[t] + jnp.where(prev >= 0, sums[jnp.maximum(prev, 0)], 0.0)
        return carry

    lax.fori_loop(0, slots, chain, 0)

    def partial(r):
        last = chain_s[0, slots + r]
        return jnp.where(last >= 0, sums[jnp.maximum(last, 0)], 0.0)

    groups = z_groups(nz)

    def send_piece(src, scales, dst, dst_scales, tx, rx, to):
        for one, other, i in ((src, dst, 0), (scales, dst_scales, 1)):
            pltpu.make_async_remote_copy(
                src_ref=one,
                dst_ref=other,
                send_sem=tx.at[i],
                recv_sem=rx.at[i],
                device_id={"gy": to},
                device_id_type=MESH,
            ).start()

    def send_y(g):
        for dy in range(1, ny):
            send_piece(
                yq.at[g, dy - 1],
                ys.at[g, dy - 1],
                yrecv.at[g, dy - 1],
                ysrecv.at[g, dy - 1],
                y_tx,
                y_rx.at[g],
                (y + dy) % ny * nz + z,
            )

    for g, dz in enumerate(groups):
        begin = (z + dz) % nz * vb

        def code_y(i, carry, g=g, begin=begin):
            dy, v = i // vb + 1, i % vb
            coded, scale = narrowed(partial((y + dy) % ny * per_y + begin + v))
            yq[g, dy - 1, v] = coded
            ys[g, dy - 1, pl.ds(v, 1), :] = scale
            return carry

        lax.fori_loop(0, (ny - 1) * vb, code_y, 0, unroll=2)
        if g:
            send_y(g - 1)
    send_y(len(groups) - 1)

    lane = lax.broadcasted_iota(jnp.int32, (1, posbuf.shape[1]), 1)
    offset = jnp.zeros((1, posbuf.shape[1]), jnp.int32)
    for c in range(peers):
        one = metabuf[c]
        rowbuf[c : c + 1, :] = one[0:1, :]
        colbuf[c : c + 1, :] = one[1:2, :]
        workbuf[c : c + 1, :] = one[2:3, :]
        posbuf[c : c + 1, :] = jnp.where(one[2:3, :] > 0, offset + lane, -1)
        offset = offset + one[3:4, :]

    lanes = posbuf.shape
    origin = 2 * lax.broadcasted_iota(jnp.int32, lanes, 0) + (
        lax.broadcasted_iota(jnp.int32, lanes, 1) >= peers
    ).astype(jnp.int32)

    def place(q, carry):
        hit = posbuf[...] == q * peers + gy

        def picked(values):
            return jnp.sum(jnp.where(hit, values, 0))

        mrow[q] = picked(rowbuf[...])
        mcol[q] = picked(colbuf[...])
        mwork[q] = picked(workbuf[...])
        source[q] = picked(origin)
        return carry

    lax.fori_loop(0, slots // 2, place, 0)

    pending = []

    def flush():
        while pending:
            hop, slot = pending.pop()
            send_piece(
                zq.at[slot],
                zs.at[slot],
                zrecv.at[slot],
                zsrecv.at[slot],
                z_tx,
                z_rx.at[slot],
                y * nz + (z + hop) % nz,
            )

    def arrived(slot):
        whole_wait(zrecv.at[slot], z_rx.at[slot, 0])
        whole_wait(zsrecv.at[slot], z_rx.at[slot, 1])

    for g, dz in enumerate(groups):
        hop, slot = z_route(dz, nz)
        whole_wait(yrecv.at[g], y_rx.at[g, 0])
        whole_wait(ysrecv.at[g], y_rx.at[g, 1])
        extra = collected(dz, nz)
        for other in extra:
            arrived(z_route(other, nz)[1])
        begin = y * per_y + (z + dz) % nz * vb
        for v in range(vb):
            total = partial(begin + v)
            for dy in range(1, ny):
                total = total + widened(yrecv[g, dy - 1, v], ysrecv[g, dy - 1, v : v + 1, :])
            for other in extra:
                at = z_route(other, nz)[1]
                total = total + widened(zrecv[at, v], zsrecv[at, v : v + 1, :])
            if dz == 0:
                prod[v] = total
            else:
                coded, scale = narrowed(total)
                zq[slot, v] = coded
                zs[slot, v : v + 1, :] = scale
        flush()
        if dz:
            pending.append((hop, slot))
    flush()
    for dz in groups:
        hop, slot = z_route(dz, nz)
        if dz and hop == dz:
            arrived(slot)
            for v in range(vb):
                prod[v] = prod[v] + widened(zrecv[slot, v], zsrecv[slot, v : v + 1, :])

    whole_wait(recvbuf.at[pl.ds(0, 2 * (peers - 1))], vals_rx)

    def settle(q, carry):
        moved[q] = recvbuf[source[q]]
        return carry

    lax.fori_loop(0, slots // 2, settle, 0, unroll=4)

    whole_wait(metabuf.at[pl.ds(0, peers - 1)], meta_tx)
    whole_wait(xbuf.at[pl.ds(0, (nx - 1) * vb)], feat_tx)
    whole_wait(recvbuf.at[pl.ds(0, 2 * (peers - 1))], vals_tx)
    whole_wait(yrecv, y_tx.at[0])
    whole_wait(ysrecv, y_tx.at[1])
    whole_wait(zrecv, z_tx.at[0])
    whole_wait(zsrecv, z_tx.at[1])


def deliver(*refs):
    count = len(refs) // 2
    outs, sems = refs[count : 2 * count], refs[-1]
    copies = [pltpu.make_async_copy(refs[i], outs[i], sems.at[i]) for i in range(count)]
    for copy in copies:
        copy.start()
    for copy in copies:
        copy.wait()


def on_device(sizes, features, tile_vals, tile_row, tile_col, tile_work):
    nx, ny, nz = sizes
    peers = ny * nz
    slots, order, _ = tile_vals.shape
    width = features.shape[1]
    vb = features.shape[0] // order
    per_y = nz * vb
    bf16, f32, i32, i16 = jnp.bfloat16, jnp.float32, jnp.int32, jnp.int16
    vmem, smem = pltpu.VMEM, pltpu.SMEM
    in_vmem, in_smem = pl.BlockSpec(memory_space=vmem), pl.BlockSpec(memory_space=smem)
    shapes = (
        jax.ShapeDtypeStruct((vb, order, width), f32),
        jax.ShapeDtypeStruct((slots // 2, order, order), bf16),
        *[jax.ShapeDtypeStruct((slots // 2,), i32)] * 3,
    )
    results = pl.pallas_call(
        functools.partial(kernel, sizes),
        out_shape=shapes,
        in_specs=[pl.BlockSpec(memory_space=pltpu.HBM)] * 8,
        out_specs=(in_vmem, in_vmem, in_smem, in_smem, in_smem),
        scratch_shapes=[
            *[smem((slots,), i32)] * 3,
            smem((1, slots + peers * vb), i32),
            *[vmem((1, slots), i32)] * 3,
            vmem((1, slots + peers * vb), i32),
            vmem((slots, order, order), bf16),
            vmem((slots, order, order), bf16),
            vmem((slots, order, order), bf16),
            vmem((nx * vb, order, width), bf16),
            vmem((slots, order, width), f32),
            vmem((peers, 8, 128), i32),
            *[vmem((peers, 128), i32)] * 4,
            vmem((nz, ny - 1, vb, order, width), i16),
            vmem((nz, ny - 1, 8, width), f32),
            vmem((nz, ny - 1, vb, order, width), i16),
            vmem((nz, ny - 1, 8, width), f32),
            vmem((nz - 1, vb, order, width), i16),
            vmem((nz - 1, 8, width), f32),
            vmem((nz - 1, vb, order, width), i16),
            vmem((nz - 1, 8, width), f32),
            smem((slots // 2,), i32),
            pltpu.SemaphoreType.DMA((15,)),
            pltpu.SemaphoreType.DMA((2,)),
            pltpu.SemaphoreType.DMA((nz, 2)),
            pltpu.SemaphoreType.DMA((2,)),
            pltpu.SemaphoreType.DMA((nz - 1, 2)),
        ],
        compiler_params=pltpu.CompilerParams(
            collective_id=0, has_side_effects=True, vmem_limit_bytes=67043328
        ),
    )(
        features.reshape(vb, order, width),
        tile_vals,
        tile_row,
        tile_col,
        tile_work,
        tile_row.reshape(1, slots),
        tile_col.reshape(1, slots),
        tile_work.reshape(1, slots),
    )
    prod, moved, mrow, mcol, mwork = pl.pallas_call(
        deliver,
        out_shape=shapes,
        in_specs=[in_vmem, in_vmem, in_smem, in_smem, in_smem],
        out_specs=[pl.BlockSpec(memory_space=pltpu.HBM)] * 5,
        scratch_shapes=[pltpu.SemaphoreType.DMA((5,))],
    )(*results)
    return prod.reshape(vb * order, width), moved, mrow, mcol, mwork


def solution(mesh):
    nx, peers = mesh.shape["gx"], mesh.shape["gy"]
    nz = min(NZ, peers // 2)
    both = ("gx", "gy")
    specs = (P(both, None), P(both, None, None), P(both), P(both), P(both))
    return jax.shard_map(
        functools.partial(on_device, (nx, peers // nz, nz)),
        mesh=mesh,
        in_specs=specs,
        out_specs=specs,
        check_vma=False,
    )
```

```python
import functools

import jax
import jax.numpy as jnp
from jax import lax
from jax.experimental import pallas as pl
from jax.experimental.pallas import tpu as pltpu
from jax.sharding import PartitionSpec as P

NZ = 8
UP = 16
AFTERY = 8
PER = 1
LIMIT = 32000.0
TINY = 1e-30
MESH = pl.DeviceIdType.MESH


def near_first(count):
    return sorted(range(1, count), key=lambda d: (min(d, count - d), d))


def tile_routes(ny, nz):
    pairs = [(dy, dz) for dy in [0, *near_first(ny)] for dz in [0, *near_first(nz)]]
    return pairs[:0:-1]


def z_groups(nz):
    half = nz // 2
    return [half, *[d for k in range(half - 1, 0, -1) for d in (nz - k, k)], 0]


def z_sends(dz, nz, vb):
    half = nz // 2
    if dz == half:
        return [(half, 1, 0, vb // 2), (0, nz - 1, vb // 2, vb - vb // 2)]
    return [(dz, 1 if dz < half else nz - 1, 0, vb)] if dz else []


def z_carried(dz, nz, vb):
    half = nz // 2
    steps = [dz + 1] if dz < half else []
    steps += [(dz - 1) % nz] if dz > half or dz == 0 else []
    found = []
    for step in steps:
        up = step == (dz + 1)
        for slot, hop, begin, count in z_sends(step, nz, vb):
            if (hop == 1) == up or nz == 2:
                found.append((slot, begin, count))
    return found if nz > 2 else found[:2]


def whole_wait(ref, sem):
    pltpu.make_async_copy(ref, ref, sem).wait()


def narrowed(value):
    peak = jnp.maximum(jnp.max(jnp.abs(value), axis=0, keepdims=True), TINY)
    coded = jnp.round(value * (LIMIT / peak)).astype(jnp.int32).astype(jnp.int16)
    return coded, peak * (1.0 / LIMIT)


def widened(coded, scale):
    return coded.astype(jnp.int32).astype(jnp.float32) * scale


def kernel(
    sizes,
    feat_hbm,
    tiles_hbm,
    row_hbm,
    col_hbm,
    work_hbm,
    row_line,
    col_line,
    work_line,
    prod,
    moved,
    mrow,
    mcol,
    mwork,
    row_s,
    col_s,
    work_s,
    chain_s,
    row_v,
    col_v,
    work_v,
    chain_v,
    tiles,
    sendbuf,
    recvbuf,
    xbuf,
    sums,
    metabuf,
    posbuf,
    cellbuf,
    workbuf,
    yq,
    ys,
    yrecv,
    ysrecv,
    ysum,
    zq,
    zs,
    zrecv,
    zsrecv,
    source,
    sems,
    y_tx,
    y_rx,
    z_tx,
    z_rx,
):
    nx, ny, nz = sizes
    peers = ny * nz
    slots = tiles.shape[0]
    vb = feat_hbm.shape[0]
    per_row = peers * vb
    per_y = nz * vb
    gx, gy = lax.axis_index("gx"), lax.axis_index("gy")
    y, z = gy // nz, gy % nz
    (tile_in, meta_tx, meta_rx, feat_tx, feat_rx, vals_tx, vals_rx) = (sems.at[i] for i in range(7))
    pass_tx, pass_rx = sems.at[15], sems.at[16]

    own_x = xbuf.at[pl.ds(gx * vb, vb)]
    small = [
        pltpu.make_async_copy(src, dst, sems.at[7 + i])
        for i, (src, dst) in enumerate(
            (
                (row_hbm, row_s),
                (row_line, row_v),
                (work_line, work_v),
                (col_line, col_v),
                (feat_hbm, own_x),
                (col_hbm, col_s),
                (work_hbm, work_s),
            )
        )
    ]
    for copy in small:
        copy.start()
    load = pltpu.make_async_copy(tiles_hbm, tiles, tile_in)
    load.start()

    barrier = pltpu.get_barrier_semaphore()

    def greet_gy(d, carry):
        pl.semaphore_signal(barrier, inc=1, device_id={"gy": (gy + d) % peers}, device_id_type=MESH)
        return carry

    def greet_gx(d, carry):
        pl.semaphore_signal(barrier, inc=1, device_id={"gx": (gx + d) % nx}, device_id_type=MESH)
        return carry

    lax.fori_loop(1, peers, greet_gy, 0)
    lax.fori_loop(1, nx, greet_gx, 0)

    for copy in small:
        copy.wait()
    live = jnp.sum((work_v[...] > 0).astype(jnp.int32), axis=1, keepdims=True)
    width = 2 * slots
    metabuf[gy, :, 0:width] = jnp.concatenate([row_v[...], col_v[...]], axis=1)
    metabuf[gy, :, width : 2 * width] = jnp.concatenate([work_v[...], work_v[...]], axis=1)
    metabuf[gy, :, 2 * width : 3 * width] = jnp.broadcast_to(live, (1, width))

    lane = lax.broadcasted_iota(jnp.int32, (1, chain_v.shape[1]), 1)
    chain_v[...] = lane - slots
    chain_v[0:1, 0:slots] = row_v[...] - gx * per_row
    wanted = chain_v[...]
    until = jnp.where(lane < slots, lane, slots)

    def link(t, latest):
        return jnp.where((wanted == row_s[t] - gx * per_row) & (t < until), t, latest)

    chain_v[...] = lax.fori_loop(0, slots, link, jnp.full(lane.shape, -1, jnp.int32), unroll=4)
    table = pltpu.make_async_copy(chain_v, chain_s, sems.at[14])
    table.start()

    pl.semaphore_wait(barrier, peers - 1 + nx - 1)

    def send_meta(d, carry):
        pltpu.make_async_remote_copy(
            src_ref=metabuf.at[gy],
            dst_ref=metabuf.at[gy],
            send_sem=meta_tx,
            recv_sem=meta_rx,
            device_id={"gy": (gy + d) % peers},
            device_id_type=MESH,
        ).start()
        return carry

    lax.fori_loop(1, peers, send_meta, 0)

    pair = gx // 2 * 2
    partner = pair + 1 - gx % 2

    def send_feat(block, to, tx, rx):
        at = xbuf.at[pl.ds(block * vb, vb)]
        pltpu.make_async_remote_copy(
            src_ref=at,
            dst_ref=at,
            send_sem=tx,
            recv_sem=rx,
            device_id={"gx": to},
            device_id_type=MESH,
        ).start()

    for d in near_first(nx // 2)[::-1]:
        send_feat(gx, (gx + 2 * d) % nx, feat_tx, feat_rx)
    send_feat(gx, partner, feat_tx, pass_rx)

    load.wait()
    whole_wait(metabuf.at[pl.ds(0, peers - 1)], meta_rx)

    def before(c, total):
        return total + jnp.where(c < gy, metabuf[c], 0)

    counted = lax.fori_loop(0, peers, before, jnp.zeros(metabuf.shape[1:], jnp.int32))
    first = jnp.max(counted[:, 2 * width : 3 * width])

    routes = tile_routes(ny, nz)

    def send_tiles(dy, dz):
        to = (y + dy) % ny * nz + (z + dz) % nz
        pltpu.make_async_remote_copy(
            src_ref=sendbuf.at[pl.ds(2 * to, 2)],
            dst_ref=recvbuf.at[pl.ds(2 * gy, 2)],
            send_sem=vals_tx,
            recv_sem=vals_rx,
            device_id={"gy": to},
            device_id_type=MESH,
        ).start()

    for i, (dy, dz) in enumerate(routes):
        to = (y + dy) % ny * nz + (z + dz) % nz
        j = (to - first) & (peers - 1)
        sendbuf[2 * to] = tiles[j]
        sendbuf[2 * to + 1] = tiles[j + peers]
        if 0 < i <= UP:
            send_tiles(*routes[i - 1])
    own = (gy - first) & (peers - 1)
    recvbuf[2 * gy] = tiles[own]
    recvbuf[2 * gy + 1] = tiles[own + peers]
    if UP >= len(routes):
        send_tiles(*routes[-1])
    held = list(routes[UP:])

    def more(n):
        for _ in range(min(n, len(held))):
            send_tiles(*held.pop(0))

    whole_wait(xbuf.at[pl.ds(0, (nx // 2 - 1) * vb)], feat_rx)
    for d in range(1, nx // 2):
        send_feat((gx + 2 * d) % nx, partner, pass_tx, pass_rx)
    table.wait()
    whole_wait(xbuf.at[pl.ds(0, nx // 2 * vb)], pass_rx)
    order = tiles.shape[1]
    pattern = lax.broadcasted_iota(jnp.int32, (order, order), 0) * order + lax.broadcasted_iota(
        jnp.int32, (order, order), 1
    )

    def multiply(t, carry):
        col = col_s[t]
        at = col // per_row * vb + col % vb
        kept = jnp.where(pattern < work_s[t], tiles[t].astype(jnp.float32), 0.0)
        product = jnp.dot(kept.astype(jnp.bfloat16), xbuf[at], preferred_element_type=jnp.float32)
        prev = chain_s[0, t]
        sums[t] = product + jnp.where(prev >= 0, sums[jnp.maximum(prev, 0)], 0.0)
        return carry

    lax.fori_loop(0, slots, multiply, 0, unroll=4)

    def partial(r):
        last = chain_s[0, slots + r]
        return jnp.where(last >= 0, sums[jnp.maximum(last, 0)], 0.0)

    groups = z_groups(nz)

    def send_piece(src, scales, dst, dst_scales, tx, rx, to):
        for one, other, i in ((src, dst, 0), (scales, dst_scales, 1)):
            pltpu.make_async_remote_copy(
                src_ref=one,
                dst_ref=other,
                send_sem=tx.at[i],
                recv_sem=rx.at[i],
                device_id={"gy": to},
                device_id_type=MESH,
            ).start()

    def send_y(g):
        for dy in range(1, ny):
            send_piece(
                yq.at[g, dy - 1],
                ys.at[g, dy - 1],
                yrecv.at[g, dy - 1],
                ysrecv.at[g, dy - 1],
                y_tx,
                y_rx.at[g],
                (y + dy) % ny * nz + z,
            )

    for g, dz in enumerate(groups):
        begin = (z + dz) % nz * vb

        def code_y(i, carry, g=g, begin=begin):
            dy, v = i // vb + 1, i % vb
            coded, scale = narrowed(partial((y + dy) % ny * per_y + begin + v))
            yq[g, dy - 1, v] = coded
            ys[g, dy - 1, pl.ds(v, 1), :] = scale
            return carry

        lax.fori_loop(0, (ny - 1) * vb, code_y, 0, unroll=2)
        if g:
            send_y(g - 1)
    send_y(len(groups) - 1)
    more(AFTERY)

    lane = lax.broadcasted_iota(jnp.int32, (1, width), 1)
    slot_of = jnp.where(lane < slots, lane, lane - slots)
    offset = jnp.zeros((1, width), jnp.int32)
    for c in range(peers):
        one = metabuf[c]
        cellbuf[c : c + 1, :] = one[:, 0:width]
        workbuf[c : c + 1, :] = one[:, width : 2 * width]
        alive = one[:, width : 2 * width] > 0
        posbuf[c : c + 1, :] = jnp.where(alive, offset + slot_of, -1)
        offset = offset + one[:, 2 * width : 3 * width]

    shape = posbuf.shape
    lanes = lax.broadcasted_iota(jnp.int32, shape, 1)
    upper = lanes >= slots
    second = jnp.where(upper, lanes - slots, lanes) >= peers
    origin = 2 * lax.broadcasted_iota(jnp.int32, shape, 0) + second.astype(jnp.int32)

    def place(q, carry):
        hit = posbuf[...] == q * peers + gy
        low, high = hit & ~upper, hit & upper

        def picked(where, values):
            return jnp.sum(jnp.where(where, values, 0))

        mrow[q] = picked(low, cellbuf[...])
        mcol[q] = picked(high, cellbuf[...])
        mwork[q] = picked(low, workbuf[...])
        source[q] = picked(low, origin)
        return carry

    lax.fori_loop(0, slots // 2, place, 0)

    def add_y(g, dz):
        whole_wait(yrecv.at[g], y_rx.at[g, 0])
        whole_wait(ysrecv.at[g], y_rx.at[g, 1])
        begin = y * per_y + (z + dz) % nz * vb
        for v in range(vb):
            total = partial(begin + v)
            for dy in range(1, ny):
                total = total + widened(yrecv[g, dy - 1, v], ysrecv[g, dy - 1, v : v + 1, :])
            ysum[g % 2, v] = total

    def send_z(dz):
        for slot, hop, begin, count in z_sends(dz, nz, vb):
            rows = pl.ds(begin, count)
            send_piece(
                zq.at[slot, rows],
                zs.at[slot],
                zrecv.at[slot, rows],
                zsrecv.at[slot],
                z_tx,
                z_rx.at[slot],
                y * nz + (z + hop) % nz,
            )

    add_y(0, groups[0])
    for g, dz in enumerate(groups):
        carried = z_carried(dz, nz, vb)
        for slot, begin, count in carried:
            whole_wait(zrecv.at[slot, pl.ds(begin, count)], z_rx.at[slot, 0])
            whole_wait(zsrecv.at[slot], z_rx.at[slot, 1])
        for v in range(vb):
            total = ysum[g % 2, v]
            for slot, begin, count in carried:
                if begin <= v < begin + count:
                    total = total + widened(zrecv[slot, v], zsrecv[slot, v : v + 1, :])
            if dz == 0:
                prod[v] = total
            else:
                coded, scale = narrowed(total)
                for slot, hop, begin, count in z_sends(dz, nz, vb):
                    if begin <= v < begin + count:
                        zq[slot, v] = coded
                        zs[slot, v : v + 1, :] = scale
        if dz:
            add_y(g + 1, groups[g + 1])
            send_z(dz)
            more(PER)

    more(99)
    whole_wait(recvbuf.at[pl.ds(0, 2 * (peers - 1))], vals_rx)

    def settle(q, carry):
        moved[q] = recvbuf[source[q]]
        return carry

    lax.fori_loop(0, slots // 2, settle, 0, unroll=4)

    whole_wait(metabuf.at[pl.ds(0, peers - 1)], meta_tx)
    whole_wait(xbuf.at[pl.ds(0, nx // 2 * vb)], feat_tx)
    whole_wait(xbuf.at[pl.ds(0, (nx // 2 - 1) * vb)], pass_tx)
    whole_wait(recvbuf.at[pl.ds(0, 2 * (peers - 1))], vals_tx)
    whole_wait(yrecv, y_tx.at[0])
    whole_wait(ysrecv, y_tx.at[1])
    whole_wait(zrecv.at[pl.ds(0, nz - 1)], z_tx.at[0])
    whole_wait(zsrecv, z_tx.at[1])


def deliver(*refs):
    count = len(refs) // 2
    outs, sems = refs[count : 2 * count], refs[-1]
    copies = [pltpu.make_async_copy(refs[i], outs[i], sems.at[i]) for i in range(count)]
    for copy in copies:
        copy.start()
    for copy in copies:
        copy.wait()


def on_device(sizes, features, tile_vals, tile_row, tile_col, tile_work):
    nx, ny, nz = sizes
    peers = ny * nz
    slots, order, _ = tile_vals.shape
    width = features.shape[1]
    vb = features.shape[0] // order
    per_y = nz * vb
    bf16, f32, i32, i16 = jnp.bfloat16, jnp.float32, jnp.int32, jnp.int16
    vmem, smem = pltpu.VMEM, pltpu.SMEM
    in_vmem, in_smem = pl.BlockSpec(memory_space=vmem), pl.BlockSpec(memory_space=smem)
    shapes = (
        jax.ShapeDtypeStruct((vb, order, width), f32),
        jax.ShapeDtypeStruct((slots // 2, order, order), bf16),
        *[jax.ShapeDtypeStruct((slots // 2,), i32)] * 3,
    )
    results = pl.pallas_call(
        functools.partial(kernel, sizes),
        out_shape=shapes,
        in_specs=[pl.BlockSpec(memory_space=pltpu.HBM)] * 8,
        out_specs=(in_vmem, in_vmem, in_smem, in_smem, in_smem),
        scratch_shapes=[
            *[smem((slots,), i32)] * 3,
            smem((1, slots + peers * vb), i32),
            *[vmem((1, slots), i32)] * 3,
            vmem((1, slots + peers * vb), i32),
            vmem((slots, order, order), bf16),
            vmem((slots, order, order), bf16),
            vmem((slots, order, order), bf16),
            vmem((nx * vb, order, width), bf16),
            vmem((slots, order, width), f32),
            vmem((peers, 1, 6 * slots), i32),
            *[vmem((peers, 2 * slots), i32)] * 3,
            vmem((nz, ny - 1, vb, order, width), i16),
            vmem((nz, ny - 1, 8, width), f32),
            vmem((nz, ny - 1, vb, order, width), i16),
            vmem((nz, ny - 1, 8, width), f32),
            vmem((2, vb, order, width), f32),
            vmem((nz, vb, order, width), i16),
            vmem((nz, 8, width), f32),
            vmem((nz, vb, order, width), i16),
            vmem((nz, 8, width), f32),
            smem((slots // 2,), i32),
            pltpu.SemaphoreType.DMA((17,)),
            pltpu.SemaphoreType.DMA((2,)),
            pltpu.SemaphoreType.DMA((nz, 2)),
            pltpu.SemaphoreType.DMA((2,)),
            pltpu.SemaphoreType.DMA((nz, 2)),
        ],
        compiler_params=pltpu.CompilerParams(
            collective_id=0, has_side_effects=True, vmem_limit_bytes=67043328
        ),
    )(
        features.reshape(vb, order, width),
        tile_vals,
        tile_row,
        tile_col,
        tile_work,
        tile_row.reshape(1, slots),
        tile_col.reshape(1, slots),
        tile_work.reshape(1, slots),
    )
    prod, moved, mrow, mcol, mwork = pl.pallas_call(
        deliver,
        out_shape=shapes,
        in_specs=[in_vmem, in_vmem, in_smem, in_smem, in_smem],
        out_specs=[pl.BlockSpec(memory_space=pltpu.HBM)] * 5,
        scratch_shapes=[pltpu.SemaphoreType.DMA((5,))],
    )(*results)
    return prod.reshape(vb * order, width), moved, mrow, mcol, mwork


def solution(mesh):
    nx, peers = mesh.shape["gx"], mesh.shape["gy"]
    nz = min(NZ, peers // 2)
    both = ("gx", "gy")
    specs = (P(both, None), P(both, None, None), P(both), P(both), P(both))
    return jax.shard_map(
        functools.partial(on_device, (nx, peers // nz, nz)),
        mesh=mesh,
        in_specs=specs,
        out_specs=specs,
        check_vma=False,
    )
```

```python
import functools

import jax
import jax.numpy as jnp
from jax import lax
from jax.experimental import pallas as pl
from jax.experimental.pallas import tpu as pltpu
from jax.sharding import PartitionSpec as P

NZ = 8
UP = 14
AFTERY = 7
PER = 2
LIMIT = 32000.0
TINY = 1e-30
MESH = pl.DeviceIdType.MESH


def near_first(count):
    return sorted(range(1, count), key=lambda d: (min(d, count - d), d))


def tile_routes(ny, nz):
    pairs = [(dy, dz) for dy in [0, *near_first(ny)] for dz in [0, *near_first(nz)]]
    return pairs[:0:-1]


def z_groups(nz):
    half = nz // 2
    return [half, *[d for k in range(half - 1, 0, -1) for d in (nz - k, k)], 0]


def z_sends(dz, nz, vb):
    half = nz // 2
    if dz == half:
        return [(half, 1, 0, vb // 2), (0, nz - 1, vb // 2, vb - vb // 2)]
    return [(dz, 1 if dz < half else nz - 1, 0, vb)] if dz else []


def z_carried(dz, nz, vb):
    half = nz // 2
    steps = [dz + 1] if dz < half else []
    steps += [(dz - 1) % nz] if dz > half or dz == 0 else []
    found = []
    for step in steps:
        up = step == (dz + 1)
        for slot, hop, begin, count in z_sends(step, nz, vb):
            if (hop == 1) == up or nz == 2:
                found.append((slot, begin, count))
    return found if nz > 2 else found[:2]


def whole_wait(ref, sem):
    pltpu.make_async_copy(ref, ref, sem).wait()


def narrowed(value):
    peak = jnp.maximum(jnp.max(jnp.abs(value), axis=0, keepdims=True), TINY)
    coded = jnp.round(value * (LIMIT / peak)).astype(jnp.int32).astype(jnp.int16)
    return coded, peak * (1.0 / LIMIT)


def widened(coded, scale):
    return coded.astype(jnp.int32).astype(jnp.float32) * scale


def kernel(
    sizes,
    feat_hbm,
    tiles_hbm,
    row_hbm,
    col_hbm,
    work_hbm,
    row_line,
    col_line,
    work_line,
    prod_hbm,
    moved_hbm,
    mrow_hbm,
    mcol_hbm,
    mwork_hbm,
    prod,
    moved,
    mrow,
    mcol,
    mwork,
    row_s,
    col_s,
    work_s,
    chain_s,
    row_v,
    col_v,
    work_v,
    chain_v,
    tiles,
    sendbuf,
    recvbuf,
    xbuf,
    sums,
    metabuf,
    posbuf,
    cellbuf,
    workbuf,
    yq,
    ys,
    yrecv,
    ysrecv,
    ysum,
    zq,
    zs,
    zrecv,
    zsrecv,
    source,
    sems,
    y_tx,
    y_rx,
    z_tx,
    z_rx,
):
    nx, ny, nz = sizes
    peers = ny * nz
    slots = tiles.shape[0]
    vb = feat_hbm.shape[0]
    per_row = peers * vb
    per_y = nz * vb
    gx, gy = lax.axis_index("gx"), lax.axis_index("gy")
    y, z = gy // nz, gy % nz
    (tile_in, meta_tx, meta_rx, feat_tx, feat_rx, vals_tx, vals_rx) = (sems.at[i] for i in range(7))
    pass_tx, pass_rx = sems.at[15], sems.at[16]

    own_x = xbuf.at[pl.ds(gx * vb, vb)]
    small = [
        pltpu.make_async_copy(src, dst, sems.at[7 + i])
        for i, (src, dst) in enumerate(
            (
                (row_hbm, row_s),
                (row_line, row_v),
                (work_line, work_v),
                (col_line, col_v),
                (feat_hbm, own_x),
                (col_hbm, col_s),
                (work_hbm, work_s),
            )
        )
    ]
    for copy in small:
        copy.start()
    load = pltpu.make_async_copy(tiles_hbm, tiles, tile_in)
    load.start()

    barrier = pltpu.get_barrier_semaphore()

    def greet_gy(d, carry):
        pl.semaphore_signal(barrier, inc=1, device_id={"gy": (gy + d) % peers}, device_id_type=MESH)
        return carry

    def greet_gx(d, carry):
        pl.semaphore_signal(barrier, inc=1, device_id={"gx": (gx + d) % nx}, device_id_type=MESH)
        return carry

    lax.fori_loop(1, peers, greet_gy, 0)
    lax.fori_loop(1, nx, greet_gx, 0)

    for copy in small:
        copy.wait()
    live = jnp.sum((work_v[...] > 0).astype(jnp.int32), axis=1, keepdims=True)
    width = 2 * slots
    metabuf[gy, :, 0:width] = jnp.concatenate([row_v[...], col_v[...]], axis=1)
    metabuf[gy, :, width : 2 * width] = jnp.concatenate([work_v[...], work_v[...]], axis=1)
    metabuf[gy, :, 2 * width : 3 * width] = jnp.broadcast_to(live, (1, width))

    lane = lax.broadcasted_iota(jnp.int32, (1, chain_v.shape[1]), 1)
    chain_v[...] = lane - slots
    chain_v[0:1, 0:slots] = row_v[...] - gx * per_row
    wanted = chain_v[...]
    until = jnp.where(lane < slots, lane, slots)

    def link(t, latest):
        return jnp.where((wanted == row_s[t] - gx * per_row) & (t < until), t, latest)

    chain_v[...] = lax.fori_loop(0, slots, link, jnp.full(lane.shape, -1, jnp.int32), unroll=4)
    table = pltpu.make_async_copy(chain_v, chain_s, sems.at[14])
    table.start()

    pl.semaphore_wait(barrier, peers - 1 + nx - 1)

    def send_meta(d, carry):
        pltpu.make_async_remote_copy(
            src_ref=metabuf.at[gy],
            dst_ref=metabuf.at[gy],
            send_sem=meta_tx,
            recv_sem=meta_rx,
            device_id={"gy": (gy + d) % peers},
            device_id_type=MESH,
        ).start()
        return carry

    lax.fori_loop(1, peers, send_meta, 0)

    pair = gx // 2 * 2
    partner = pair + 1 - gx % 2

    def send_feat(block, to, tx, rx):
        at = xbuf.at[pl.ds(block * vb, vb)]
        pltpu.make_async_remote_copy(
            src_ref=at,
            dst_ref=at,
            send_sem=tx,
            recv_sem=rx,
            device_id={"gx": to},
            device_id_type=MESH,
        ).start()

    for d in near_first(nx // 2)[::-1]:
        send_feat(gx, (gx + 2 * d) % nx, feat_tx, feat_rx)
    send_feat(gx, partner, feat_tx, pass_rx)

    load.wait()
    whole_wait(metabuf.at[pl.ds(0, peers - 1)], meta_rx)

    def before(c, total):
        return total + jnp.where(c < gy, metabuf[c], 0)

    counted = lax.fori_loop(0, peers, before, jnp.zeros(metabuf.shape[1:], jnp.int32))
    first = jnp.max(counted[:, 2 * width : 3 * width])

    routes = tile_routes(ny, nz)

    def send_tiles(dy, dz):
        to = (y + dy) % ny * nz + (z + dz) % nz
        pltpu.make_async_remote_copy(
            src_ref=sendbuf.at[pl.ds(2 * to, 2)],
            dst_ref=recvbuf.at[pl.ds(2 * gy, 2)],
            send_sem=vals_tx,
            recv_sem=vals_rx,
            device_id={"gy": to},
            device_id_type=MESH,
        ).start()

    for i, (dy, dz) in enumerate(routes):
        to = (y + dy) % ny * nz + (z + dz) % nz
        j = (to - first) & (peers - 1)
        sendbuf[2 * to] = tiles[j]
        sendbuf[2 * to + 1] = tiles[j + peers]
        if 0 < i <= UP:
            send_tiles(*routes[i - 1])
    own = (gy - first) & (peers - 1)
    recvbuf[2 * gy] = tiles[own]
    recvbuf[2 * gy + 1] = tiles[own + peers]
    if UP >= len(routes):
        send_tiles(*routes[-1])
    held = list(routes[UP:])

    def more(n):
        for _ in range(min(n, len(held))):
            send_tiles(*held.pop(0))

    whole_wait(xbuf.at[pl.ds(0, (nx // 2 - 1) * vb)], feat_rx)
    for d in range(1, nx // 2):
        send_feat((gx + 2 * d) % nx, partner, pass_tx, pass_rx)
    table.wait()
    whole_wait(xbuf.at[pl.ds(0, nx // 2 * vb)], pass_rx)
    order = tiles.shape[1]
    pattern = lax.broadcasted_iota(jnp.int32, (order, order), 0) * order + lax.broadcasted_iota(
        jnp.int32, (order, order), 1
    )

    def multiply(t, carry):
        col = col_s[t]
        at = col // per_row * vb + col % vb
        kept = jnp.where(pattern < work_s[t], tiles[t].astype(jnp.float32), 0.0)
        product = jnp.dot(kept.astype(jnp.bfloat16), xbuf[at], preferred_element_type=jnp.float32)
        prev = chain_s[0, t]
        sums[t] = product + jnp.where(prev >= 0, sums[jnp.maximum(prev, 0)], 0.0)
        return carry

    lax.fori_loop(0, slots, multiply, 0, unroll=4)

    def partial(r):
        last = chain_s[0, slots + r]
        return jnp.where(last >= 0, sums[jnp.maximum(last, 0)], 0.0)

    groups = z_groups(nz)

    def send_piece(src, scales, dst, dst_scales, tx, rx, to):
        for one, other, i in ((src, dst, 0), (scales, dst_scales, 1)):
            pltpu.make_async_remote_copy(
                src_ref=one,
                dst_ref=other,
                send_sem=tx.at[i],
                recv_sem=rx.at[i],
                device_id={"gy": to},
                device_id_type=MESH,
            ).start()

    def send_y(g):
        for dy in range(1, ny):
            send_piece(
                yq.at[g, dy - 1],
                ys.at[g, dy - 1],
                yrecv.at[g, dy - 1],
                ysrecv.at[g, dy - 1],
                y_tx,
                y_rx.at[g],
                (y + dy) % ny * nz + z,
            )

    for g, dz in enumerate(groups):
        begin = (z + dz) % nz * vb

        def code_y(i, carry, g=g, begin=begin):
            dy, v = i // vb + 1, i % vb
            coded, scale = narrowed(partial((y + dy) % ny * per_y + begin + v))
            yq[g, dy - 1, v] = coded
            ys[g, dy - 1, pl.ds(v, 1), :] = scale
            return carry

        lax.fori_loop(0, (ny - 1) * vb, code_y, 0, unroll=2)
        if g:
            send_y(g - 1)
    send_y(len(groups) - 1)
    more(AFTERY)

    lane = lax.broadcasted_iota(jnp.int32, (1, width), 1)
    slot_of = jnp.where(lane < slots, lane, lane - slots)
    offset = jnp.zeros((1, width), jnp.int32)
    for c in range(peers):
        one = metabuf[c]
        cellbuf[c : c + 1, :] = one[:, 0:width]
        workbuf[c : c + 1, :] = one[:, width : 2 * width]
        alive = one[:, width : 2 * width] > 0
        posbuf[c : c + 1, :] = jnp.where(alive, offset + slot_of, -1)
        offset = offset + one[:, 2 * width : 3 * width]

    shape = posbuf.shape
    lanes = lax.broadcasted_iota(jnp.int32, shape, 1)
    upper = lanes >= slots
    second = jnp.where(upper, lanes - slots, lanes) >= peers
    origin = 2 * lax.broadcasted_iota(jnp.int32, shape, 0) + second.astype(jnp.int32)

    def place(q, carry):
        hit = posbuf[...] == q * peers + gy
        low, high = hit & ~upper, hit & upper

        def picked(where, values):
            return jnp.sum(jnp.where(where, values, 0))

        mrow[q] = picked(low, cellbuf[...])
        mcol[q] = picked(high, cellbuf[...])
        mwork[q] = picked(low, workbuf[...])
        source[q] = picked(low, origin)
        return carry

    lax.fori_loop(0, slots // 2, place, 0)
    leaving = [
        pltpu.make_async_copy(src, dst, sems.at[17 + i])
        for i, (src, dst) in enumerate(((mrow, mrow_hbm), (mcol, mcol_hbm), (mwork, mwork_hbm)))
    ]
    for copy in leaving:
        copy.start()

    def add_y(g, dz):
        whole_wait(yrecv.at[g], y_rx.at[g, 0])
        whole_wait(ysrecv.at[g], y_rx.at[g, 1])
        begin = y * per_y + (z + dz) % nz * vb
        for v in range(vb):
            total = partial(begin + v)
            for dy in range(1, ny):
                total = total + widened(yrecv[g, dy - 1, v], ysrecv[g, dy - 1, v : v + 1, :])
            ysum[g % 2, v] = total

    def send_z(dz):
        for slot, hop, begin, count in z_sends(dz, nz, vb):
            rows = pl.ds(begin, count)
            send_piece(
                zq.at[slot, rows],
                zs.at[slot],
                zrecv.at[slot, rows],
                zsrecv.at[slot],
                z_tx,
                z_rx.at[slot],
                y * nz + (z + hop) % nz,
            )

    add_y(0, groups[0])
    for g, dz in enumerate(groups):
        carried = z_carried(dz, nz, vb)
        for slot, begin, count in carried:
            whole_wait(zrecv.at[slot, pl.ds(begin, count)], z_rx.at[slot, 0])
            whole_wait(zsrecv.at[slot], z_rx.at[slot, 1])
        for v in range(vb):
            total = ysum[g % 2, v]
            for slot, begin, count in carried:
                if begin <= v < begin + count:
                    total = total + widened(zrecv[slot, v], zsrecv[slot, v : v + 1, :])
            if dz == 0:
                prod[v] = total
            else:
                coded, scale = narrowed(total)
                for slot, hop, begin, count in z_sends(dz, nz, vb):
                    if begin <= v < begin + count:
                        zq[slot, v] = coded
                        zs[slot, v : v + 1, :] = scale
        if dz:
            add_y(g + 1, groups[g + 1])
            send_z(dz)
            more(PER)

    leaving.append(pltpu.make_async_copy(prod, prod_hbm, sems.at[20]))
    leaving[-1].start()
    more(99)
    whole_wait(recvbuf.at[pl.ds(0, 2 * (peers - 1))], vals_rx)

    def settle(q, carry):
        moved[q] = recvbuf[source[q]]
        return carry

    batch = slots // 8
    for i in range(4):
        lax.fori_loop(i * batch, (i + 1) * batch, settle, 0, unroll=2)
        rows = pl.ds(i * batch, batch)
        leaving.append(pltpu.make_async_copy(moved.at[rows], moved_hbm.at[rows], sems.at[21 + i]))
        leaving[-1].start()

    whole_wait(metabuf.at[pl.ds(0, peers - 1)], meta_tx)
    whole_wait(xbuf.at[pl.ds(0, nx // 2 * vb)], feat_tx)
    whole_wait(xbuf.at[pl.ds(0, (nx // 2 - 1) * vb)], pass_tx)
    whole_wait(recvbuf.at[pl.ds(0, 2 * (peers - 1))], vals_tx)
    whole_wait(yrecv, y_tx.at[0])
    whole_wait(ysrecv, y_tx.at[1])
    whole_wait(zrecv.at[pl.ds(0, nz - 1)], z_tx.at[0])
    whole_wait(zsrecv, z_tx.at[1])
    for copy in leaving:
        copy.wait()


def deliver(*refs):
    ins, outs, held, in_sems, out_sems = refs[:5], refs[5:10], refs[10:15], refs[15], refs[16]
    batch = ins[1].shape[0] // 4
    steps = [(i, slice(None)) for i in (0, 2, 3, 4)]
    steps = [(1, pl.ds(g * batch, batch)) for g in range(4)] + steps
    arriving, leaving = [], []
    for n, (i, rows) in enumerate(steps):
        arriving.append(pltpu.make_async_copy(ins[i].at[rows], held[i].at[rows], in_sems.at[n]))
        leaving.append(pltpu.make_async_copy(held[i].at[rows], outs[i].at[rows], out_sems.at[n]))
        arriving[-1].start()
    for arrive, leave in zip(arriving, leaving, strict=True):
        arrive.wait()
        leave.start()
    for leave in leaving:
        leave.wait()


def on_device(sizes, features, tile_vals, tile_row, tile_col, tile_work):
    nx, ny, nz = sizes
    peers = ny * nz
    slots, order, _ = tile_vals.shape
    width = features.shape[1]
    vb = features.shape[0] // order
    per_y = nz * vb
    bf16, f32, i32, i16 = jnp.bfloat16, jnp.float32, jnp.int32, jnp.int16
    vmem, smem = pltpu.VMEM, pltpu.SMEM
    in_hbm = pl.BlockSpec(memory_space=pltpu.HBM)
    results_held = [
        vmem((vb, order, width), f32),
        vmem((slots // 2, order, order), bf16),
        *[smem((slots // 2,), i32)] * 3,
    ]
    shapes = (
        jax.ShapeDtypeStruct((vb, order, width), f32),
        jax.ShapeDtypeStruct((slots // 2, order, order), bf16),
        *[jax.ShapeDtypeStruct((slots // 2,), i32)] * 3,
    )
    results = pl.pallas_call(
        functools.partial(kernel, sizes),
        out_shape=shapes,
        in_specs=[in_hbm] * 8,
        out_specs=[in_hbm] * 5,
        scratch_shapes=[
            *results_held,
            *[smem((slots,), i32)] * 3,
            smem((1, slots + peers * vb), i32),
            *[vmem((1, slots), i32)] * 3,
            vmem((1, slots + peers * vb), i32),
            vmem((slots, order, order), bf16),
            vmem((slots, order, order), bf16),
            vmem((slots, order, order), bf16),
            vmem((nx * vb, order, width), bf16),
            vmem((slots, order, width), f32),
            vmem((peers, 1, 6 * slots), i32),
            *[vmem((peers, 2 * slots), i32)] * 3,
            vmem((nz, ny - 1, vb, order, width), i16),
            vmem((nz, ny - 1, 8, width), f32),
            vmem((nz, ny - 1, vb, order, width), i16),
            vmem((nz, ny - 1, 8, width), f32),
            vmem((2, vb, order, width), f32),
            vmem((nz, vb, order, width), i16),
            vmem((nz, 8, width), f32),
            vmem((nz, vb, order, width), i16),
            vmem((nz, 8, width), f32),
            smem((slots // 2,), i32),
            pltpu.SemaphoreType.DMA((25,)),
            pltpu.SemaphoreType.DMA((2,)),
            pltpu.SemaphoreType.DMA((nz, 2)),
            pltpu.SemaphoreType.DMA((2,)),
            pltpu.SemaphoreType.DMA((nz, 2)),
        ],
        compiler_params=pltpu.CompilerParams(
            collective_id=0, has_side_effects=True, vmem_limit_bytes=67043328
        ),
    )(
        features.reshape(vb, order, width),
        tile_vals,
        tile_row,
        tile_col,
        tile_work,
        tile_row.reshape(1, slots),
        tile_col.reshape(1, slots),
        tile_work.reshape(1, slots),
    )
    prod, moved, mrow, mcol, mwork = pl.pallas_call(
        deliver,
        out_shape=shapes,
        in_specs=[in_hbm] * 5,
        out_specs=[in_hbm] * 5,
        scratch_shapes=[*results_held, *[pltpu.SemaphoreType.DMA((8,))] * 2],
    )(*results)
    return prod.reshape(vb * order, width), moved, mrow, mcol, mwork


def solution(mesh):
    nx, peers = mesh.shape["gx"], mesh.shape["gy"]
    nz = min(NZ, peers // 2)
    both = ("gx", "gy")
    specs = (P(both, None), P(both, None, None), P(both), P(both), P(both))
    return jax.shard_map(
        functools.partial(on_device, (nx, peers // nz, nz)),
        mesh=mesh,
        in_specs=specs,
        out_specs=specs,
        check_vma=False,
    )
```

```python
import functools

import jax
import jax.numpy as jnp
from jax import lax
from jax.experimental import pallas as pl
from jax.experimental.pallas import tpu as pltpu
from jax.sharding import PartitionSpec as P

NZ = 8
UP = 14
AFTERY = 7
PER = 2
LIMIT = 32000.0
TINY = 1e-30
MESH = pl.DeviceIdType.MESH


def near_first(count):
    return sorted(range(1, count), key=lambda d: (min(d, count - d), d))


def tile_routes(ny, nz):
    pairs = [(dy, dz) for dy in [0, *near_first(ny)] for dz in [0, *near_first(nz)]]
    return pairs[:0:-1]


def z_groups(nz):
    half = nz // 2
    return [half, *[d for k in range(half - 1, 0, -1) for d in (nz - k, k)], 0]


def z_sends(dz, nz, vb):
    half = nz // 2
    if dz == half:
        return [(half, 1, 0, vb // 2), (0, nz - 1, vb // 2, vb - vb // 2)]
    return [(dz, 1 if dz < half else nz - 1, 0, vb)] if dz else []


def z_carried(dz, nz, vb):
    half = nz // 2
    steps = [dz + 1] if dz < half else []
    steps += [(dz - 1) % nz] if dz > half or dz == 0 else []
    found = []
    for step in steps:
        up = step == (dz + 1)
        for slot, hop, begin, count in z_sends(step, nz, vb):
            if (hop == 1) == up or nz == 2:
                found.append((slot, begin, count))
    return found if nz > 2 else found[:2]


def whole_wait(ref, sem):
    pltpu.make_async_copy(ref, ref, sem).wait()


def narrowed(value):
    peak = jnp.maximum(jnp.max(jnp.abs(value), axis=0, keepdims=True), TINY)
    coded = jnp.round(value * (LIMIT / peak)).astype(jnp.int32).astype(jnp.int16)
    return coded, peak * (1.0 / LIMIT)


def widened(coded, scale):
    return coded.astype(jnp.int32).astype(jnp.float32) * scale


def kernel(
    sizes,
    feat_hbm,
    tiles_hbm,
    row_hbm,
    col_hbm,
    work_hbm,
    row_line,
    col_line,
    work_line,
    prod_hbm,
    moved_hbm,
    mrow_hbm,
    mcol_hbm,
    mwork_hbm,
    prod,
    moved,
    mrow,
    mcol,
    mwork,
    row_s,
    col_s,
    work_s,
    chain_s,
    row_v,
    col_v,
    work_v,
    chain_v,
    tiles,
    sendbuf,
    recvbuf,
    xbuf,
    sums,
    metabuf,
    posbuf,
    cellbuf,
    workbuf,
    yq,
    ys,
    yrecv,
    ysrecv,
    ysum,
    zq,
    zs,
    zrecv,
    zsrecv,
    source,
    sems,
    y_tx,
    y_rx,
    z_tx,
    z_rx,
):
    nx, ny, nz = sizes
    peers = ny * nz
    slots = tiles.shape[0]
    vb = feat_hbm.shape[0]
    per_row = peers * vb
    per_y = nz * vb
    gx, gy = lax.axis_index("gx"), lax.axis_index("gy")
    y, z = gy // nz, gy % nz
    (tile_in, meta_tx, meta_rx, feat_tx, feat_rx, vals_tx, vals_rx) = (sems.at[i] for i in range(7))
    pass_tx, pass_rx = sems.at[15], sems.at[16]

    own_x = xbuf.at[pl.ds(gx * vb, vb)]
    small = [
        pltpu.make_async_copy(src, dst, sems.at[7 + i])
        for i, (src, dst) in enumerate(
            (
                (row_hbm, row_s),
                (row_line, row_v),
                (work_line, work_v),
                (col_line, col_v),
                (feat_hbm, own_x),
                (col_hbm, col_s),
                (work_hbm, work_s),
            )
        )
    ]
    for copy in small:
        copy.start()
    load = pltpu.make_async_copy(tiles_hbm, tiles, tile_in)
    load.start()

    barrier = pltpu.get_barrier_semaphore()

    def greet_gy(d, carry):
        pl.semaphore_signal(barrier, inc=1, device_id={"gy": (gy + d) % peers}, device_id_type=MESH)
        return carry

    def greet_gx(d, carry):
        pl.semaphore_signal(barrier, inc=1, device_id={"gx": (gx + d) % nx}, device_id_type=MESH)
        return carry

    lax.fori_loop(1, peers, greet_gy, 0)
    lax.fori_loop(1, nx, greet_gx, 0)

    for copy in small:
        copy.wait()
    live = jnp.sum((work_v[...] > 0).astype(jnp.int32), axis=1, keepdims=True)
    width = 2 * slots
    metabuf[gy, :, 0:width] = jnp.concatenate([row_v[...], col_v[...]], axis=1)
    metabuf[gy, :, width : 2 * width] = jnp.concatenate([work_v[...], work_v[...]], axis=1)
    metabuf[gy, :, 2 * width : 3 * width] = jnp.broadcast_to(live, (1, width))

    lane = lax.broadcasted_iota(jnp.int32, (1, chain_v.shape[1]), 1)
    chain_v[...] = lane - slots
    chain_v[0:1, 0:slots] = row_v[...] - gx * per_row
    wanted = chain_v[...]
    until = jnp.where(lane < slots, lane, slots)

    def link(t, latest):
        return jnp.where((wanted == row_s[t] - gx * per_row) & (t < until), t, latest)

    chain_v[...] = lax.fori_loop(0, slots, link, jnp.full(lane.shape, -1, jnp.int32), unroll=4)
    table = pltpu.make_async_copy(chain_v, chain_s, sems.at[14])
    table.start()

    pl.semaphore_wait(barrier, peers - 1 + nx - 1)

    def send_meta(d, carry):
        pltpu.make_async_remote_copy(
            src_ref=metabuf.at[gy],
            dst_ref=metabuf.at[gy],
            send_sem=meta_tx,
            recv_sem=meta_rx,
            device_id={"gy": (gy + d) % peers},
            device_id_type=MESH,
        ).start()
        return carry

    lax.fori_loop(1, peers, send_meta, 0)

    pair = gx // 2 * 2
    partner = pair + 1 - gx % 2

    def send_feat(block, to, tx, rx):
        at = xbuf.at[pl.ds(block * vb, vb)]
        pltpu.make_async_remote_copy(
            src_ref=at,
            dst_ref=at,
            send_sem=tx,
            recv_sem=rx,
            device_id={"gx": to},
            device_id_type=MESH,
        ).start()

    for d in near_first(nx // 2)[::-1]:
        send_feat(gx, (gx + 2 * d) % nx, feat_tx, feat_rx)
    send_feat(gx, partner, feat_tx, pass_rx)

    load.wait()
    whole_wait(metabuf.at[pl.ds(0, peers - 1)], meta_rx)

    def before(c, total):
        return total + jnp.where(c < gy, metabuf[c], 0)

    counted = lax.fori_loop(0, peers, before, jnp.zeros(metabuf.shape[1:], jnp.int32))
    first = jnp.max(counted[:, 2 * width : 3 * width])

    routes = tile_routes(ny, nz)

    def send_tiles(dy, dz):
        to = (y + dy) % ny * nz + (z + dz) % nz
        pltpu.make_async_remote_copy(
            src_ref=sendbuf.at[pl.ds(2 * to, 2)],
            dst_ref=recvbuf.at[pl.ds(2 * gy, 2)],
            send_sem=vals_tx,
            recv_sem=vals_rx,
            device_id={"gy": to},
            device_id_type=MESH,
        ).start()

    for i, (dy, dz) in enumerate(routes):
        to = (y + dy) % ny * nz + (z + dz) % nz
        j = (to - first) & (peers - 1)
        sendbuf[2 * to] = tiles[j]
        sendbuf[2 * to + 1] = tiles[j + peers]
        if 0 < i <= UP:
            send_tiles(*routes[i - 1])
    own = (gy - first) & (peers - 1)
    recvbuf[2 * gy] = tiles[own]
    recvbuf[2 * gy + 1] = tiles[own + peers]
    if UP >= len(routes):
        send_tiles(*routes[-1])
    held = list(routes[UP:])

    def more(n):
        for _ in range(min(n, len(held))):
            send_tiles(*held.pop(0))

    whole_wait(xbuf.at[pl.ds(0, (nx // 2 - 1) * vb)], feat_rx)
    for d in range(1, nx // 2):
        send_feat((gx + 2 * d) % nx, partner, pass_tx, pass_rx)
    table.wait()
    whole_wait(xbuf.at[pl.ds(0, nx // 2 * vb)], pass_rx)
    order = tiles.shape[1]
    pattern = lax.broadcasted_iota(jnp.int32, (order, order), 0) * order + lax.broadcasted_iota(
        jnp.int32, (order, order), 1
    )

    def multiply(t, carry):
        col = col_s[t]
        at = col // per_row * vb + col % vb
        kept = jnp.where(pattern < work_s[t], tiles[t].astype(jnp.float32), 0.0)
        product = jnp.dot(kept.astype(jnp.bfloat16), xbuf[at], preferred_element_type=jnp.float32)
        prev = chain_s[0, t]
        sums[t] = product + jnp.where(prev >= 0, sums[jnp.maximum(prev, 0)], 0.0)
        return carry

    lax.fori_loop(0, slots, multiply, 0, unroll=8)

    def partial(r):
        last = chain_s[0, slots + r]
        return jnp.where(last >= 0, sums[jnp.maximum(last, 0)], 0.0)

    groups = z_groups(nz)

    def send_piece(src, scales, dst, dst_scales, tx, rx, to):
        for one, other, i in ((src, dst, 0), (scales, dst_scales, 1)):
            pltpu.make_async_remote_copy(
                src_ref=one,
                dst_ref=other,
                send_sem=tx.at[i],
                recv_sem=rx.at[i],
                device_id={"gy": to},
                device_id_type=MESH,
            ).start()

    def send_y(g):
        for dy in range(1, ny):
            send_piece(
                yq.at[g, dy - 1],
                ys.at[g, dy - 1],
                yrecv.at[g, dy - 1],
                ysrecv.at[g, dy - 1],
                y_tx,
                y_rx.at[g],
                (y + dy) % ny * nz + z,
            )

    for g, dz in enumerate(groups):
        begin = (z + dz) % nz * vb

        def code_y(i, carry, g=g, begin=begin):
            dy, v = i // vb + 1, i % vb
            coded, scale = narrowed(partial((y + dy) % ny * per_y + begin + v))
            yq[g, dy - 1, v] = coded
            ys[g, dy - 1, pl.ds(v, 1), :] = scale
            return carry

        lax.fori_loop(0, (ny - 1) * vb, code_y, 0, unroll=6)
        if g:
            send_y(g - 1)
    send_y(len(groups) - 1)
    more(AFTERY)

    lane = lax.broadcasted_iota(jnp.int32, (1, width), 1)
    slot_of = jnp.where(lane < slots, lane, lane - slots)
    offset = jnp.zeros((1, width), jnp.int32)
    for c in range(peers):
        one = metabuf[c]
        cellbuf[c : c + 1, :] = one[:, 0:width]
        workbuf[c : c + 1, :] = one[:, width : 2 * width]
        alive = one[:, width : 2 * width] > 0
        posbuf[c : c + 1, :] = jnp.where(alive, offset + slot_of, -1)
        offset = offset + one[:, 2 * width : 3 * width]

    shape = posbuf.shape
    lanes = lax.broadcasted_iota(jnp.int32, shape, 1)
    upper = lanes >= slots
    second = jnp.where(upper, lanes - slots, lanes) >= peers
    origin = 2 * lax.broadcasted_iota(jnp.int32, shape, 0) + second.astype(jnp.int32)

    def place(q, carry):
        hit = posbuf[...] == q * peers + gy
        low, high = hit & ~upper, hit & upper

        def picked(where, values):
            return jnp.sum(jnp.where(where, values, 0))

        mrow[q] = picked(low, cellbuf[...])
        mcol[q] = picked(high, cellbuf[...])
        mwork[q] = picked(low, workbuf[...])
        source[q] = picked(low, origin)
        return carry

    lax.fori_loop(0, slots // 2, place, 0)
    leaving = [
        pltpu.make_async_copy(src, dst, sems.at[17 + i])
        for i, (src, dst) in enumerate(((mrow, mrow_hbm), (mcol, mcol_hbm), (mwork, mwork_hbm)))
    ]
    for copy in leaving:
        copy.start()

    def add_y(g, dz):
        whole_wait(yrecv.at[g], y_rx.at[g, 0])
        whole_wait(ysrecv.at[g], y_rx.at[g, 1])
        begin = y * per_y + (z + dz) % nz * vb
        for v in range(vb):
            total = partial(begin + v)
            for dy in range(1, ny):
                total = total + widened(yrecv[g, dy - 1, v], ysrecv[g, dy - 1, v : v + 1, :])
            ysum[g % 2, v] = total

    def send_z(dz):
        for slot, hop, begin, count in z_sends(dz, nz, vb):
            rows = pl.ds(begin, count)
            send_piece(
                zq.at[slot, rows],
                zs.at[slot],
                zrecv.at[slot, rows],
                zsrecv.at[slot],
                z_tx,
                z_rx.at[slot],
                y * nz + (z + hop) % nz,
            )

    add_y(0, groups[0])
    for g, dz in enumerate(groups):
        carried = z_carried(dz, nz, vb)
        for slot, begin, count in carried:
            whole_wait(zrecv.at[slot, pl.ds(begin, count)], z_rx.at[slot, 0])
            whole_wait(zsrecv.at[slot], z_rx.at[slot, 1])
        for v in range(vb):
            total = ysum[g % 2, v]
            for slot, begin, count in carried:
                if begin <= v < begin + count:
                    total = total + widened(zrecv[slot, v], zsrecv[slot, v : v + 1, :])
            if dz == 0:
                prod[v] = total
            else:
                coded, scale = narrowed(total)
                for slot, hop, begin, count in z_sends(dz, nz, vb):
                    if begin <= v < begin + count:
                        zq[slot, v] = coded
                        zs[slot, v : v + 1, :] = scale
        if dz:
            add_y(g + 1, groups[g + 1])
            send_z(dz)
            more(PER)

    leaving.append(pltpu.make_async_copy(prod, prod_hbm, sems.at[20]))
    leaving[-1].start()
    more(99)
    whole_wait(recvbuf.at[pl.ds(0, 2 * (peers - 1))], vals_rx)

    def settle(q, carry):
        moved[q] = recvbuf[source[q]]
        return carry

    batch = slots // 8
    for i in range(4):
        lax.fori_loop(i * batch, (i + 1) * batch, settle, 0, unroll=2)
        rows = pl.ds(i * batch, batch)
        leaving.append(pltpu.make_async_copy(moved.at[rows], moved_hbm.at[rows], sems.at[21 + i]))
        leaving[-1].start()

    whole_wait(metabuf.at[pl.ds(0, peers - 1)], meta_tx)
    whole_wait(xbuf.at[pl.ds(0, nx // 2 * vb)], feat_tx)
    whole_wait(xbuf.at[pl.ds(0, (nx // 2 - 1) * vb)], pass_tx)
    whole_wait(recvbuf.at[pl.ds(0, 2 * (peers - 1))], vals_tx)
    whole_wait(yrecv, y_tx.at[0])
    whole_wait(ysrecv, y_tx.at[1])
    whole_wait(zrecv.at[pl.ds(0, nz - 1)], z_tx.at[0])
    whole_wait(zsrecv, z_tx.at[1])
    for copy in leaving:
        copy.wait()


def deliver(*refs):
    ins, outs, held, in_sems, out_sems = refs[:5], refs[5:10], refs[10:15], refs[15], refs[16]
    batch = ins[1].shape[0] // 4
    steps = [(i, slice(None)) for i in (0, 2, 3, 4)]
    steps = [(1, pl.ds(g * batch, batch)) for g in range(4)] + steps
    arriving, leaving = [], []
    for n, (i, rows) in enumerate(steps):
        arriving.append(pltpu.make_async_copy(ins[i].at[rows], held[i].at[rows], in_sems.at[n]))
        leaving.append(pltpu.make_async_copy(held[i].at[rows], outs[i].at[rows], out_sems.at[n]))
        arriving[-1].start()
    for arrive, leave in zip(arriving, leaving, strict=True):
        arrive.wait()
        leave.start()
    for leave in leaving:
        leave.wait()


def on_device(sizes, features, tile_vals, tile_row, tile_col, tile_work):
    nx, ny, nz = sizes
    peers = ny * nz
    slots, order, _ = tile_vals.shape
    width = features.shape[1]
    vb = features.shape[0] // order
    per_y = nz * vb
    bf16, f32, i32, i16 = jnp.bfloat16, jnp.float32, jnp.int32, jnp.int16
    vmem, smem = pltpu.VMEM, pltpu.SMEM
    in_hbm = pl.BlockSpec(memory_space=pltpu.HBM)
    results_held = [
        vmem((vb, order, width), f32),
        vmem((slots // 2, order, order), bf16),
        *[smem((slots // 2,), i32)] * 3,
    ]
    shapes = (
        jax.ShapeDtypeStruct((vb, order, width), f32),
        jax.ShapeDtypeStruct((slots // 2, order, order), bf16),
        *[jax.ShapeDtypeStruct((slots // 2,), i32)] * 3,
    )
    results = pl.pallas_call(
        functools.partial(kernel, sizes),
        out_shape=shapes,
        in_specs=[in_hbm] * 8,
        out_specs=[in_hbm] * 5,
        scratch_shapes=[
            *results_held,
            *[smem((slots,), i32)] * 3,
            smem((1, slots + peers * vb), i32),
            *[vmem((1, slots), i32)] * 3,
            vmem((1, slots + peers * vb), i32),
            vmem((slots, order, order), bf16),
            vmem((slots, order, order), bf16),
            vmem((slots, order, order), bf16),
            vmem((nx * vb, order, width), bf16),
            vmem((slots, order, width), f32),
            vmem((peers, 1, 6 * slots), i32),
            *[vmem((peers, 2 * slots), i32)] * 3,
            vmem((nz, ny - 1, vb, order, width), i16),
            vmem((nz, ny - 1, 8, width), f32),
            vmem((nz, ny - 1, vb, order, width), i16),
            vmem((nz, ny - 1, 8, width), f32),
            vmem((2, vb, order, width), f32),
            vmem((nz, vb, order, width), i16),
            vmem((nz, 8, width), f32),
            vmem((nz, vb, order, width), i16),
            vmem((nz, 8, width), f32),
            smem((slots // 2,), i32),
            pltpu.SemaphoreType.DMA((25,)),
            pltpu.SemaphoreType.DMA((2,)),
            pltpu.SemaphoreType.DMA((nz, 2)),
            pltpu.SemaphoreType.DMA((2,)),
            pltpu.SemaphoreType.DMA((nz, 2)),
        ],
        compiler_params=pltpu.CompilerParams(
            collective_id=0, has_side_effects=True, vmem_limit_bytes=67043328
        ),
    )(
        features.reshape(vb, order, width),
        tile_vals,
        tile_row,
        tile_col,
        tile_work,
        tile_row.reshape(1, slots),
        tile_col.reshape(1, slots),
        tile_work.reshape(1, slots),
    )
    prod, moved, mrow, mcol, mwork = pl.pallas_call(
        deliver,
        out_shape=shapes,
        in_specs=[in_hbm] * 5,
        out_specs=[in_hbm] * 5,
        scratch_shapes=[*results_held, *[pltpu.SemaphoreType.DMA((8,))] * 2],
    )(*results)
    return prod.reshape(vb * order, width), moved, mrow, mcol, mwork


def solution(mesh):
    nx, peers = mesh.shape["gx"], mesh.shape["gy"]
    nz = min(NZ, peers // 2)
    both = ("gx", "gy")
    specs = (P(both, None), P(both, None, None), P(both), P(both), P(both))
    return jax.shard_map(
        functools.partial(on_device, (nx, peers // nz, nz)),
        mesh=mesh,
        in_specs=specs,
        out_specs=specs,
        check_vma=False,
    )
```
